32 devices in a mesh: groups: 2 (over y), ctx: 4 (over z), head: 2 (over x), rep: 2 (over core).
Axes of the slice: x: 2, y: 2, z: 4, core: 2. Of those that a mesh axis runs over, the one named last changes fastest.
Arguments:
- queries: bfloat16 [2048, 4096], P(('groups', 'ctx'), ('head', 'rep')), parts along dimension 0, may hold values from -24 to 24
- keys: bfloat16 [2048, 1024], P(('groups', 'ctx'), ('head', 'rep')), parts along dimension 0, may hold values from -6 to 6
- values: bfloat16 [2048, 1024], P(('groups', 'ctx'), ('head', 'rep')), parts along dimension 0, may hold values from -6 to 6
- span_order: int32 [8], replicated, may hold values from 0 to 7, as said below
Outputs:
- attended: bfloat16 [2048, 4096], P(('groups', 'ctx'), ('head', 'rep')), parts along dimension 0
The draws below stay inside these ranges and needn't reach their ends.
There are 2 independent parts, one for each index of `groups`. The reference program is written for one: setup_inputs(seed, part) draws one part's arguments, and reference() takes and returns one part's arrays. A program takes and returns all parts, laid end to end along the dimension named above; an argument that names none is the same for every part. Nothing has to cross between parts.
Inputs may be any that keep to these rules, and one draw needn't show every extreme that they name: `span_order`: A permutation of the spans in which entries 2 d and 2 d + 1 are c and 7 - c for some c.
All inputs are finite; a program needn't handle non-finite values.
Results may differ from the reference program's by a relative error of at most 0.0047.
Values may be sent and summed in bfloat16 or wider, within the bound.
A program may use at most 64 MiB of HBM per device.

```python
import math
import jax
import jax.numpy as jnp
from jax import lax

QUERY_HEADS = 32
KEY_VALUE_HEADS = 8
HEAD_SIZE = 128
SPAN = 128
SPANS = 8
SEQUENCE_TOKENS = 1024


def draw_queries(key, part):
    perturb_random_key = jax.random.fold_in(key, 21)
    scale_key = jax.random.fold_in(key, 22)
    noise = jax.random.truncated_normal(perturb_random_key, -4.0, 4.0, (SEQUENCE_TOKENS, QUERY_HEADS, HEAD_SIZE), jnp.float32)
    row_scale = jnp.exp(jax.random.uniform(scale_key, (SEQUENCE_TOKENS, QUERY_HEADS, 1), jnp.float32, 0.0, math.log(6.0)))
    sampled_values = noise * row_scale
    return sampled_values.reshape(SEQUENCE_TOKENS, QUERY_HEADS * HEAD_SIZE).astype(jnp.bfloat16)


def draw_keys(key, part):
    perturb_random_key = jax.random.fold_in(key, 31)
    sampled_values = jax.random.truncated_normal(perturb_random_key, -6.0, 6.0, (SEQUENCE_TOKENS, KEY_VALUE_HEADS, HEAD_SIZE), jnp.float32)
    return sampled_values.reshape(SEQUENCE_TOKENS, KEY_VALUE_HEADS * HEAD_SIZE).astype(jnp.bfloat16)


def draw_span_order(key, part):
    pair_count = SPANS // 2
    pair_order = jax.random.permutation(jax.random.fold_in(key, 41), pair_count)
    flip_bits = jax.random.randint(jax.random.fold_in(key, 42), (pair_count,), 0, 2)
    first_span = jnp.where(flip_bits == 1, pair_order, SPANS - 1 - pair_order)
    second_span = SPANS - 1 - first_span
    return jnp.stack([first_span, second_span], axis=1).reshape(SPANS).astype(jnp.int32)


def block_levels(key, extent, pieces, low, high):
    factor_of = 1.0
    for axis_at, blocks in pieces:
        steps = jax.random.uniform(jax.random.fold_in(jax.random.fold_in(key, 6), axis_at), (blocks,), jnp.float32, low / len(pieces), high / len(pieces))
        factor_of = factor_of * jnp.repeat(jnp.exp(steps), extent[axis_at] // blocks).reshape((-1,) + (1,) * (len(extent) - 1 - axis_at))
    return factor_of


def bell_draw(stream_key, shape, scale, most, cuts=(), kind=jnp.bfloat16):
    result = jax.random.normal(stream_key, shape, jnp.float32) * scale
    if len(cuts) > 0:
        result = block_levels(stream_key, shape, cuts, -0.22, 0.18) * result
    return jnp.clip(result, min=-most, max=most).astype(kind)


def setup_inputs(seed: int = 0, part: int = 0) -> dict:
    arg_keys = jax.random.split(jax.random.key(seed), 5)
    part_keys = jax.random.split(jax.random.fold_in(arg_keys[4], part), 5)
    queries = draw_queries(jax.random.fold_in(jax.random.fold_in(arg_keys[4], part), 71), part)
    keys = draw_keys(jax.random.fold_in(jax.random.fold_in(arg_keys[4], part), 71), part)
    values = bell_draw(part_keys[2], (SEQUENCE_TOKENS, KEY_VALUE_HEADS * HEAD_SIZE), 1.0, 6.0, ((0, 4), (1, 4)))
    span_order = draw_span_order(jax.random.fold_in(arg_keys[4], 71), part)
    return {"queries": queries, "keys": keys, "values": values, "span_order": span_order}


masked_score = -1e+30

def source_partials(query_block, query_pos, key_block, value_block, key_pos):
    score_scale = 1.0 / math.sqrt(HEAD_SIZE)
    scores = jnp.einsum('rhgd,shd->rhgs', query_block, key_block) * score_scale
    allowed = (key_pos[None, :] <= query_pos[:, None])[:, None, None, :]
    masked = jnp.where(allowed, scores, masked_score)
    row_top = lax.optimization_barrier(jnp.max(masked, axis=-1))
    weights = jnp.where(allowed, jnp.exp(masked - row_top[..., None]), 0.0)
    row_total = lax.optimization_barrier(jnp.sum(weights, axis=-1))
    rounded = lax.optimization_barrier(weights.astype(jnp.bfloat16)).astype(jnp.float32)
    numerator = jnp.einsum('rhgs,shd->rhgd', rounded, value_block)
    partial_value = numerator / jnp.maximum(row_total, 1.0)[..., None]
    partial_value = lax.optimization_barrier(partial_value.astype(jnp.bfloat16)).astype(jnp.float32)
    return (partial_value, row_top, row_total)

def reference(queries, keys, values, span_order):
    row_index = jnp.arange(SEQUENCE_TOKENS, dtype=jnp.int32)
    positions = span_order[row_index // SPAN].astype(jnp.int32) * SPAN + row_index % SPAN
    contributor_list = SPANS // 2
    rows_per_block = 2 * SPAN
    common_values = QUERY_HEADS // KEY_VALUE_HEADS
    query_block_list = queries.astype(jnp.float32).reshape(contributor_list, rows_per_block, KEY_VALUE_HEADS, common_values, HEAD_SIZE)
    key_block_list = keys.astype(jnp.float32).reshape(contributor_list, rows_per_block, KEY_VALUE_HEADS, HEAD_SIZE)
    value_block_list = values.astype(jnp.float32).reshape(contributor_list, rows_per_block, KEY_VALUE_HEADS, HEAD_SIZE)
    position_blocks = positions.reshape(contributor_list, rows_per_block)

    def one_block(operands):
        query_block, query_pos = operands

        def one_source(inputs_now):
            return source_partials(query_block, query_pos, inputs_now[0], inputs_now[1], inputs_now[2])
        partials, row_tops, row_totals = lax.map(one_source, (key_block_list, value_block_list, position_blocks))
        best_top = lax.optimization_barrier(jnp.max(row_tops, axis=0))
        source_weight = row_totals * jnp.exp(row_tops - best_top[None])
        weighted = lax.optimization_barrier(jnp.sum(source_weight[..., None] * partials, axis=0))
        return (weighted / lax.optimization_barrier(jnp.sum(source_weight, axis=0))[..., None]).astype(jnp.bfloat16)
    attended = lax.map(one_block, (query_block_list, position_blocks))
    return attended.reshape(SEQUENCE_TOKENS, QUERY_HEADS * HEAD_SIZE)
```

```python
import functools
import math

import jax
import jax.numpy as jnp
from jax import lax
from jax.experimental import pallas as pl
from jax.experimental.pallas import tpu as pltpu
from jax.sharding import PartitionSpec as P

HEAD_SIZE = 128
MASKED = -1e30
MESH = pl.DeviceIdType.MESH
KEY, VALUE = 0, 1


def attend(
    n, order_hbm, q_hbm, k_hbm, v_hbm, out_ref,
    order_ref, q_ref, k_ref, v_ref, stack_ref, p_ref, top_ref, sum_ref, acc_ref,
    load_sem, send_sem, recv_sem,
):
    me = lax.axis_index("ctx")
    rows, q_cols = q_ref.shape
    span = rows // 2
    kv_heads = k_ref.shape[1]
    group = q_cols // HEAD_SIZE // kv_heads
    tall = group * span
    exponent_scale = math.log2(math.e) / math.sqrt(HEAD_SIZE)
    buffers = (k_ref, v_ref)
    chunks = [(kind, head) for head in range(kv_heads) for kind in (KEY, VALUE)]

    def columns(head):
        return pl.ds(head * HEAD_SIZE, HEAD_SIZE)

    loads = {
        (kind, head): pltpu.make_async_copy(
            (k_hbm, v_hbm)[kind].at[:, columns(head)], buffers[kind].at[me, head], load_sem.at[2 * head + kind]
        )
        for kind, head in chunks
    }
    load_order = pltpu.make_async_copy(order_hbm, order_ref, load_sem.at[2 * kv_heads])
    load_q = pltpu.make_async_copy(q_hbm, q_ref, load_sem.at[2 * kv_heads + 1])
    for chunk in chunks:
        loads[chunk].start()
    load_q.start()
    load_order.start()

    major = jnp.where(me < n // 2, -1, 1)

    def inside(index):
        return (index >= 0) & (index < n)

    barrier = pltpu.get_barrier_semaphore()
    for way in (-1, 1):
        @pl.when(inside(me + way))
        def _():
            pl.semaphore_signal(barrier, inc=1, device_id={"ctx": me + way}, device_id_type=MESH)

    pl.semaphore_wait(barrier, jnp.where(me > 0, 1, 0) + jnp.where(me < n - 1, 1, 0))

    def hop(way, kind, head, step, block):
        lane = (way + 1) // 2
        return pltpu.make_async_remote_copy(
            src_ref=buffers[kind].at[block, head],
            dst_ref=buffers[kind].at[block, head],
            send_sem=send_sem.at[lane, kind, head, step],
            recv_sem=recv_sem.at[lane, kind, head, step],
            device_id={"ctx": jnp.clip(me + way, 0, n - 1)},
            device_id_type=MESH,
        )

    def arrive(way, kind, head, step):
        hop(way, kind, head, step - 1, me - way * step).wait_recv()

        @pl.when(inside(me + way))
        def _():
            hop(way, kind, head, step, me - way * step).start()

    for kind, head in chunks:
        loads[kind, head].wait()
        for way in (major, -major):
            @pl.when(inside(me + way))
            def _():
                hop(way, kind, head, 0, me).start()

    load_q.wait()
    load_order.wait()

    def low_first(block):
        return order_ref[2 * block] < order_ref[2 * block + 1]

    def low_span(block):
        return jnp.minimum(order_ref[2 * block], order_ref[2 * block + 1])

    def low_high(ref, block, head):
        first, second = ref[block, head, :span], ref[block, head, span:]
        swap = low_first(block)
        return jnp.where(swap, first, second), jnp.where(swap, second, first)

    def score(queries, keys):
        return lax.dot_general(
            queries, keys, (((1,), (1,)), ((), ())), preferred_element_type=jnp.float32
        )

    def peak(scores):
        return jnp.broadcast_to(jnp.max(scores, axis=1, keepdims=True), (tall, HEAD_SIZE))

    def weights_of(scores, top):
        return jnp.exp2((scores - top) * exponent_scale).astype(jnp.bfloat16)

    mine_first = low_first(me)

    def stored(low, high):
        return jnp.where(mine_first, low, high), jnp.where(mine_first, high, low)

    def mixer(earlier, low, high):
        none = jnp.zeros_like(low)
        to_low = jnp.concatenate([none, jnp.where(earlier, low, none)], axis=0)
        to_high = jnp.concatenate([low, jnp.where(earlier, none, high)], axis=0)
        return jnp.concatenate(stored(to_low, to_high), axis=1)

    def product(weights, values):
        return jnp.dot(weights, values, preferred_element_type=jnp.float32)

    for head in range(kv_heads):
        for member in range(group):
            column = columns(head * group + member)
            low, high = stored(q_ref[:span, column], q_ref[span:, column])
            stack_ref[head, 0, member * span : (member + 1) * span] = low
            stack_ref[head, 1, member * span : (member + 1) * span] = high

    row = lax.rem(lax.broadcasted_iota(jnp.int32, (tall, span), 0), span)
    bias = jnp.where(lax.broadcasted_iota(jnp.int32, (tall, span), 1) <= row, 0.0, MASKED)
    ones = jnp.ones((span, HEAD_SIZE), jnp.bfloat16)
    for head in range(kv_heads):
        key_low, key_high = low_high(k_ref, me, head)
        value_low, value_high = low_high(v_ref, me, head)
        low = score(stack_ref[head, 0], key_low) + bias
        low_top = peak(low)
        top_ref[head, 0] = low_top
        low = weights_of(low, low_top)
        cross = score(stack_ref[head, 1], key_low)
        high = score(stack_ref[head, 1], key_high) + bias
        high_top = jnp.maximum(peak(cross), peak(high))
        top_ref[head, 1] = high_top
        high = jnp.concatenate([weights_of(cross, high_top), weights_of(high, high_top)], axis=1)
        low = product(low, jnp.concatenate([value_low, ones], axis=1))
        high = product(high, jnp.concatenate(
            [jnp.concatenate([value_low, value_high], axis=0), jnp.concatenate([ones, ones], axis=0)], axis=1
        ))
        acc_ref[head] = jnp.concatenate(stored(low[:, :HEAD_SIZE], high[:, :HEAD_SIZE]), axis=1)
        sum_ref[head] = jnp.concatenate(stored(low[:, HEAD_SIZE:], high[:, HEAD_SIZE:]), axis=1)

    def weigh(block, head):
        earlier = low_span(block) < low_span(me)
        key_low, key_high = low_high(k_ref, block, head)
        cross = score(stack_ref[head, 1], key_low)
        other = score(
            jnp.where(earlier, stack_ref[head, 0], stack_ref[head, 1]),
            jnp.where(earlier, key_low, key_high),
        )
        other_top = peak(other)
        old_low, old_high = top_ref[head, 0], top_ref[head, 1]
        low_top = jnp.maximum(old_low, jnp.where(earlier, other_top, MASKED))
        high_top = jnp.maximum(
            jnp.maximum(old_high, peak(cross)), jnp.where(earlier, MASKED, other_top)
        )
        top_ref[head, 0] = low_top
        top_ref[head, 1] = high_top
        weights = jnp.concatenate(
            [weights_of(cross, high_top), weights_of(other, jnp.where(earlier, low_top, high_top))], axis=1
        )
        p_ref[head] = weights
        fade = jnp.concatenate(
            stored(
                jnp.exp2((old_low - low_top) * exponent_scale),
                jnp.exp2((old_high - high_top) * exponent_scale),
            ),
            axis=1,
        )
        acc_ref[head] *= fade
        sum_ref[head] = sum_ref[head] * fade + product(weights, mixer(earlier, ones, ones))

    def gathered(block, head):
        earlier = low_span(block) < low_span(me)
        return acc_ref[head] + product(p_ref[head], mixer(earlier, *low_high(v_ref, block, head)))

    def turn(step, head):
        for way in (major, -major):
            @pl.when(inside(me - way * step))
            def _():
                arrive(way, KEY, head, step)
                weigh(me - way * step, head)
                arrive(way, VALUE, head, step)
                acc_ref[head] = gathered(me - way * step, head)

    def steps(step, carry):
        for head in range(kv_heads):
            turn(step, head)
        return carry

    lax.fori_loop(1, n - 1, steps, 0)

    def finish(head, total):
        result = (total * sum_ref[head]).astype(out_ref.dtype)
        for member in range(group):
            column = columns(head * group + member)
            part = slice(member * span, (member + 1) * span)
            out_ref[:span, column] = result[part, :HEAD_SIZE]
            out_ref[span:, column] = result[part, HEAD_SIZE:]

    last = me - major * (n - 1)
    for head in range(kv_heads):
        @pl.when(inside(last))
        def _():
            hop(major, KEY, head, n - 2, last).wait_recv()
            weigh(last, head)
            sum_ref[head] = 1.0 / sum_ref[head]
            hop(major, VALUE, head, n - 2, last).wait_recv()
            finish(head, gathered(last, head))

        @pl.when(jnp.logical_not(inside(last)))
        def _():
            sum_ref[head] = 1.0 / sum_ref[head]
            finish(head, acc_ref[head])

    def drain(step, carry):
        for kind, head in chunks:
            for way in (major, -major):
                @pl.when(inside(me - way * step) & inside(me + way))
                def _():
                    hop(way, kind, head, step, me - way * step).wait_send()
        return carry

    lax.fori_loop(0, n - 1, drain, 0)


def shards(n, queries, keys, values, span_order):
    rows, q_cols = queries.shape
    span = rows // 2
    kv_heads = keys.shape[1] // HEAD_SIZE
    tall = q_cols // HEAD_SIZE // kv_heads * span
    inputs = [pltpu.with_memory_space_constraint(x, pltpu.HBM) for x in (span_order, queries, keys, values)]
    return pl.pallas_call(
        functools.partial(attend, n),
        out_shape=jax.ShapeDtypeStruct((rows, q_cols), jnp.bfloat16),
        in_specs=[pl.BlockSpec(memory_space=pltpu.HBM)] * 4,
        out_specs=pl.BlockSpec(memory_space=pltpu.VMEM),
        scratch_shapes=[
            pltpu.SMEM(span_order.shape, jnp.int32),
            pltpu.VMEM((rows, q_cols), jnp.bfloat16),
            pltpu.VMEM((n, kv_heads, rows, HEAD_SIZE), jnp.bfloat16),
            pltpu.VMEM((n, kv_heads, rows, HEAD_SIZE), jnp.bfloat16),
            pltpu.VMEM((kv_heads, 2, tall, HEAD_SIZE), jnp.bfloat16),
            pltpu.VMEM((kv_heads, tall, 2 * span), jnp.bfloat16),
            pltpu.VMEM((kv_heads, 2, tall, HEAD_SIZE), jnp.float32),
            pltpu.VMEM((kv_heads, tall, 2 * HEAD_SIZE), jnp.float32),
            pltpu.VMEM((kv_heads, tall, 2 * HEAD_SIZE), jnp.float32),
            pltpu.SemaphoreType.DMA((2 * kv_heads + 2,)),
            pltpu.SemaphoreType.DMA((2, 2, kv_heads, n)),
            pltpu.SemaphoreType.DMA((2, 2, kv_heads, n)),
        ],
        compiler_params=pltpu.CompilerParams(
            collective_id=0, has_side_effects=True, vmem_limit_bytes=32 * 2**20
        ),
    )(*inputs)


def solution(mesh):
    split = P(("groups", "ctx"), ("head", "rep"))
    return jax.shard_map(
        functools.partial(shards, mesh.shape["ctx"]),
        mesh=mesh,
        in_specs=(split, split, split, P()),
        out_specs=split,
        check_vma=False,
    )
```

```python
import functools
import math

import jax
import jax.numpy as jnp
from jax import lax
from jax.experimental import pallas as pl
from jax.experimental.pallas import tpu as pltpu
from jax.sharding import PartitionSpec as P

HEAD_SIZE = 128
MASKED = -1e30
MESH = pl.DeviceIdType.MESH
KEY, VALUE = 0, 1
OWN, RELAYED = 0, 1


def attend(
    n, order_hbm, q_hbm, k_hbm, v_hbm, out_ref,
    order_ref, q_ref, kv_ref, stack_ref, p_ref, top_ref, sum_ref, acc_ref,
    chunk_sem, load_sem, send_sem, entered_sem,
):
    me = lax.axis_index("ctx")
    rows, q_cols = q_ref.shape
    span = rows // 2
    per_block = kv_ref.shape[0] // n
    kv_heads = per_block // 2
    group = q_cols // HEAD_SIZE // kv_heads
    tall = group * span
    exponent_scale = math.log2(math.e) / math.sqrt(HEAD_SIZE)
    chunks = [(kind, head) for head in range(kv_heads) for kind in (KEY, VALUE)]

    def columns(head):
        return pl.ds(head * HEAD_SIZE, HEAD_SIZE)

    def place(kind, head, block):
        return block * per_block + 2 * head + kind

    loads = [
        pltpu.make_async_copy(
            (k_hbm, v_hbm)[kind].at[:, columns(head)],
            kv_ref.at[place(kind, head, me)],
            chunk_sem.at[place(kind, head, me)],
        )
        for kind, head in chunks
    ]
    load_order = pltpu.make_async_copy(order_hbm, order_ref, load_sem.at[0])
    load_q = pltpu.make_async_copy(q_hbm, q_ref, load_sem.at[1])
    for load in loads:
        load.start()
    load_q.start()
    load_order.start()

    major = jnp.where(me < n // 2, -1, 1)

    def inside(index):
        return (index >= 0) & (index < n)

    barrier = pltpu.get_barrier_semaphore()

    @pl.when(me < n - 1)
    def _():
        pl.semaphore_signal(barrier, inc=1, device_id={"ctx": me + 1}, device_id_type=MESH)

    @pl.when(me > 0)
    def _():
        pl.semaphore_wait(barrier, 1)
        pl.semaphore_signal(entered_sem, inc=1, device_id={"ctx": me - 1}, device_id_type=MESH)

    def send(way, at, pool, count=None):
        part = kv_ref.at[at] if count is None else kv_ref.at[pl.ds(at, count)]
        return pltpu.make_async_remote_copy(
            src_ref=part,
            dst_ref=part,
            send_sem=send_sem.at[pool],
            recv_sem=chunk_sem.at[at],
            device_id={"ctx": jnp.clip(me + way, 0, n - 1)},
            device_id_type=MESH,
        )

    def take(way, kind, head, step):
        send(-way, place(kind, head, me - way * step), RELAYED).wait_recv()

    def arrive(way, kind, head, step):
        take(way, kind, head, step)

        @pl.when(inside(me + way))
        def _():
            send(way, place(kind, head, me - way * step), RELAYED).start()

    for load, (kind, head) in zip(loads, chunks):
        load.wait()

        @pl.when(me > 0)
        def _():
            send(-1, place(kind, head, me), OWN).start()

    @pl.when(me < n - 1)
    def _():
        pl.semaphore_wait(entered_sem, 1)
        for kind, head in chunks:
            send(1, place(kind, head, me), OWN).start()

    load_q.wait()
    load_order.wait()

    def low_first(block):
        return order_ref[2 * block] < order_ref[2 * block + 1]

    def low_span(block):
        return jnp.minimum(order_ref[2 * block], order_ref[2 * block + 1])

    def low_high(kind, block, head):
        at = place(kind, head, block)
        first, second = kv_ref[at, :span], kv_ref[at, span:]
        swap = low_first(block)
        return jnp.where(swap, first, second), jnp.where(swap, second, first)

    def score(queries, keys):
        return lax.dot_general(
            queries, keys, (((1,), (1,)), ((), ())), preferred_element_type=jnp.float32
        )

    def peak(scores):
        return jnp.broadcast_to(jnp.max(scores, axis=1, keepdims=True), (tall, HEAD_SIZE))

    def weights_of(scores, top):
        return jnp.exp2((scores - top) * exponent_scale).astype(jnp.bfloat16)

    mine_first = low_first(me)

    def stored(low, high):
        return jnp.where(mine_first, low, high), jnp.where(mine_first, high, low)

    def mixer(earlier, low, high):
        none = jnp.zeros_like(low)
        to_low = jnp.concatenate([none, jnp.where(earlier, low, none)], axis=0)
        to_high = jnp.concatenate([low, jnp.where(earlier, none, high)], axis=0)
        return jnp.concatenate(stored(to_low, to_high), axis=1)

    def product(weights, values):
        return jnp.dot(weights, values, preferred_element_type=jnp.float32)

    for head in range(kv_heads):
        for member in range(group):
            column = columns(head * group + member)
            low, high = stored(q_ref[:span, column], q_ref[span:, column])
            stack_ref[head, 0, member * span : (member + 1) * span] = low
            stack_ref[head, 1, member * span : (member + 1) * span] = high

    row = lax.rem(lax.broadcasted_iota(jnp.int32, (tall, span), 0), span)
    bias = jnp.where(lax.broadcasted_iota(jnp.int32, (tall, span), 1) <= row, 0.0, MASKED)
    ones = jnp.ones((span, HEAD_SIZE), jnp.bfloat16)
    for head in range(kv_heads):
        key_low, key_high = low_high(KEY, me, head)
        value_low, value_high = low_high(VALUE, me, head)
        low = score(stack_ref[head, 0], key_low) + bias
        low_top = peak(low)
        top_ref[head, 0] = low_top
        low = weights_of(low, low_top)
        cross = score(stack_ref[head, 1], key_low)
        high = score(stack_ref[head, 1], key_high) + bias
        high_top = jnp.maximum(peak(cross), peak(high))
        top_ref[head, 1] = high_top
        high = jnp.concatenate([weights_of(cross, high_top), weights_of(high, high_top)], axis=1)
        low = product(low, jnp.concatenate([value_low, ones], axis=1))
        high = product(high, jnp.concatenate(
            [jnp.concatenate([value_low, value_high], axis=0), jnp.concatenate([ones, ones], axis=0)], axis=1
        ))
        acc_ref[head] = jnp.concatenate(stored(low[:, :HEAD_SIZE], high[:, :HEAD_SIZE]), axis=1)
        sum_ref[head] = jnp.concatenate(stored(low[:, HEAD_SIZE:], high[:, HEAD_SIZE:]), axis=1)

    def weigh(block, head):
        earlier = low_span(block) < low_span(me)
        key_low, key_high = low_high(KEY, block, head)
        cross = score(stack_ref[head, 1], key_low)
        other = score(
            jnp.where(earlier, stack_ref[head, 0], stack_ref[head, 1]),
            jnp.where(earlier, key_low, key_high),
        )
        other_top = peak(other)
        old_low, old_high = top_ref[head, 0], top_ref[head, 1]
        low_top = jnp.maximum(old_low, jnp.where(earlier, other_top, MASKED))
        high_top = jnp.maximum(
            jnp.maximum(old_high, peak(cross)), jnp.where(earlier, MASKED, other_top)
        )
        top_ref[head, 0] = low_top
        top_ref[head, 1] = high_top
        weights = jnp.concatenate(
            [weights_of(cross, high_top), weights_of(other, jnp.where(earlier, low_top, high_top))], axis=1
        )
        p_ref[head] = weights
        fade = jnp.concatenate(
            stored(
                jnp.exp2((old_low - low_top) * exponent_scale),
                jnp.exp2((old_high - high_top) * exponent_scale),
            ),
            axis=1,
        )
        acc_ref[head] *= fade
        sum_ref[head] = sum_ref[head] * fade + product(weights, mixer(earlier, ones, ones))

    def gathered(block, head):
        earlier = low_span(block) < low_span(me)
        return acc_ref[head] + product(p_ref[head], mixer(earlier, *low_high(VALUE, block, head)))

    def turn(step, head):
        for way in (major, -major):
            @pl.when(inside(me - way * step))
            def _():
                arrive(way, KEY, head, step)
                weigh(me - way * step, head)
                arrive(way, VALUE, head, step)
                acc_ref[head] = gathered(me - way * step, head)

    def steps(step, carry):
        for head in range(kv_heads):
            turn(step, head)
        return carry

    lax.fori_loop(1, n - 1, steps, 0)

    def finish(head, total):
        result = (total * sum_ref[head]).astype(out_ref.dtype)
        for member in range(group):
            column = columns(head * group + member)
            part = slice(member * span, (member + 1) * span)
            out_ref[:span, column] = result[part, :HEAD_SIZE]
            out_ref[span:, column] = result[part, HEAD_SIZE:]

    last = me - major * (n - 1)
    for head in range(kv_heads):
        @pl.when(inside(last))
        def _():
            take(major, KEY, head, n - 1)
            weigh(last, head)
            sum_ref[head] = 1.0 / sum_ref[head]
            take(major, VALUE, head, n - 1)
            finish(head, gathered(last, head))

        @pl.when(jnp.logical_not(inside(last)))
        def _():
            sum_ref[head] = 1.0 / sum_ref[head]
            finish(head, acc_ref[head])

    @pl.when((me > 0) & (me < n - 1))
    def _():
        send(1, 0, OWN, 2 * per_block).wait_send()
        send(1, 0, RELAYED, (n - 1) * per_block).wait_send()

    @pl.when((me == 0) | (me == n - 1))
    def _():
        send(1, 0, OWN, per_block).wait_send()


def shards(n, queries, keys, values, span_order):
    rows, q_cols = queries.shape
    span = rows // 2
    kv_heads = keys.shape[1] // HEAD_SIZE
    tall = q_cols // HEAD_SIZE // kv_heads * span
    inputs = [pltpu.with_memory_space_constraint(x, pltpu.HBM) for x in (span_order, queries, keys, values)]
    return pl.pallas_call(
        functools.partial(attend, n),
        out_shape=jax.ShapeDtypeStruct((rows, q_cols), jnp.bfloat16),
        in_specs=[pl.BlockSpec(memory_space=pltpu.HBM)] * 4,
        out_specs=pl.BlockSpec(memory_space=pltpu.VMEM),
        scratch_shapes=[
            pltpu.SMEM(span_order.shape, jnp.int32),
            pltpu.VMEM((rows, q_cols), jnp.bfloat16),
            pltpu.VMEM((2 * kv_heads * n, rows, HEAD_SIZE), jnp.bfloat16),
            pltpu.VMEM((kv_heads, 2, tall, HEAD_SIZE), jnp.bfloat16),
            pltpu.VMEM((kv_heads, tall, 2 * span), jnp.bfloat16),
            pltpu.VMEM((kv_heads, 2, tall, HEAD_SIZE), jnp.float32),
            pltpu.VMEM((kv_heads, tall, 2 * HEAD_SIZE), jnp.float32),
            pltpu.VMEM((kv_heads, tall, 2 * HEAD_SIZE), jnp.float32),
            pltpu.SemaphoreType.DMA((2 * kv_heads * n,)),
            pltpu.SemaphoreType.DMA((2,)),
            pltpu.SemaphoreType.DMA((2,)),
            pltpu.SemaphoreType.REGULAR,
        ],
        compiler_params=pltpu.CompilerParams(
            collective_id=0, has_side_effects=True, vmem_limit_bytes=32 * 2**20
        ),
    )(*inputs)


def solution(mesh):
    split = P(("groups", "ctx"), ("head", "rep"))
    return jax.shard_map(
        functools.partial(shards, mesh.shape["ctx"]),
        mesh=mesh,
        in_specs=(split, split, split, P()),
        out_specs=split,
        check_vma=False,
    )
```

```python
import functools
import math

import jax
import jax.numpy as jnp
from jax import lax
from jax.experimental import pallas as pl
from jax.experimental.pallas import tpu as pltpu
from jax.sharding import PartitionSpec as P

HEAD_SIZE = 128
MASKED = -1e30
MESH = pl.DeviceIdType.MESH
KEY, VALUE = 0, 1
SIDES = ("groups", "head")
ROUTES = ((1, 0), (0, 1), (1, 1))
OWN, RELAYED, DETOURED, PARTIAL = 0, 1, 2, 3


def attend(
    n, sides, order_hbm, q_hbm, k_hbm, v_hbm, out_ref,
    order_ref, q_ref, kv_ref, detour_ref, stack_ref, p_ref, top_ref, sum_ref, acc_ref,
    chunk_sem, load_sem, send_sem, detour_sem, entered_sem,
):
    me = lax.axis_index("ctx")
    rows, q_cols = q_ref.shape
    span = rows // 2
    per_block = kv_ref.shape[0] // n
    kv_heads = per_block // 2
    group = q_cols // HEAD_SIZE // kv_heads
    tall = group * span
    exponent_scale = math.log2(math.e) / math.sqrt(HEAD_SIZE)
    chunks = [(kind, head) for head in range(kv_heads) for kind in (KEY, VALUE)]

    def columns(head):
        return pl.ds(head * HEAD_SIZE, HEAD_SIZE)

    def place(kind, head, block):
        return block * per_block + 2 * head + kind

    loads = [
        pltpu.make_async_copy(
            (k_hbm, v_hbm)[kind].at[:, columns(head)],
            kv_ref.at[place(kind, head, me)],
            chunk_sem.at[place(kind, head, me)],
        )
        for kind, head in chunks
    ]
    load_order = pltpu.make_async_copy(order_hbm, order_ref, load_sem.at[0])
    load_q = pltpu.make_async_copy(q_hbm, q_ref, load_sem.at[1])
    load_order.start()
    for load in loads:
        load.start()

    major = jnp.where(me < n // 2, -1, 1)

    def inside(index):
        return (index >= 0) & (index < n)

    barrier = pltpu.get_barrier_semaphore()

    @pl.when(me < n - 1)
    def _():
        pl.semaphore_signal(barrier, inc=1, device_id={"ctx": me + 1}, device_id_type=MESH)

    core = lax.axis_index("rep")

    def on_line(route):
        return (lax.axis_index(SIDES[0]) == route[0]) & (lax.axis_index(SIDES[1]) == route[1])

    def via(route):
        return {SIDES[0]: route[0], SIDES[1]: route[1], "rep": 1}

    corner = on_line((0, 0)) & (core == 0)
    source = corner & (me == n - 1)
    spared = corner & (me == 1)
    beside = [on_line(route) & (core == 1) & (me == n - 1) for route in ROUTES]
    if sides:
        @pl.when(corner & (me == 0))
        def _():
            for route in ROUTES:
                pl.semaphore_signal(
                    barrier, inc=1, device_id={"ctx": n - 1, **via(route)}, device_id_type=MESH
                )

        @pl.when(beside[0] | beside[1] | beside[2])
        def _():
            pl.semaphore_signal(
                barrier, inc=1, device_id={"groups": 0, "head": 0, "rep": 0}, device_id_type=MESH
            )

    @pl.when(me > 0)
    def _():
        helpers = jnp.where(source, len(ROUTES), jnp.where(beside[0] | beside[1] | beside[2], 1, 0))
        pl.semaphore_wait(barrier, 1 + helpers if sides else 1)
        pl.semaphore_signal(entered_sem, inc=1, device_id={"ctx": me - 1}, device_id_type=MESH)

    def send(way, at, pool, count=None):
        part = kv_ref.at[at] if count is None else kv_ref.at[pl.ds(at, count)]
        return pltpu.make_async_remote_copy(
            src_ref=part,
            dst_ref=part,
            send_sem=send_sem.at[pool],
            recv_sem=chunk_sem.at[at],
            device_id={"ctx": jnp.clip(me + way, 0, n - 1)},
            device_id_type=MESH,
        )

    def take(way, kind, head, step):
        send(-way, place(kind, head, me - way * step), RELAYED).wait_recv()

    half = rows // 2
    pieces = [(KEY, 0), (KEY, half), (VALUE, 0)]

    def far_part(kind, start):
        return kv_ref.at[place(kind, kv_heads - 1, n - 1), pl.ds(start, half)]

    def divert(i):
        return pltpu.make_async_remote_copy(
            src_ref=far_part(*pieces[i]),
            dst_ref=detour_ref,
            send_sem=send_sem.at[PARTIAL if pieces[i][0] == VALUE else DETOURED],
            recv_sem=detour_sem,
            device_id=via(ROUTES[i]),
            device_id_type=MESH,
        )

    def rejoin(i):
        return pltpu.make_async_remote_copy(
            src_ref=detour_ref,
            dst_ref=far_part(*pieces[i]),
            send_sem=send_sem.at[DETOURED],
            recv_sem=chunk_sem.at[place(pieces[i][0], kv_heads - 1, n - 1)],
            device_id={"ctx": 0, "groups": 0, "head": 0, "rep": 0},
            device_id_type=MESH,
        )

    def remainder():
        return pltpu.make_async_remote_copy(
            src_ref=far_part(VALUE, half),
            dst_ref=far_part(VALUE, half),
            send_sem=send_sem.at[PARTIAL],
            recv_sem=chunk_sem.at[place(VALUE, kv_heads - 1, n - 1)],
            device_id={"ctx": 0},
            device_id_type=MESH,
        )

    def arrive(way, kind, head, step, leading):
        take(way, kind, head, step)
        onward = inside(me + way)
        if sides and leading and head == kv_heads - 1:
            last = spared & (step == n - 2)
            onward &= jnp.logical_not(last)
            if kind == VALUE:
                @pl.when(last)
                def _():
                    remainder().start()

        @pl.when(onward)
        def _():
            send(way, place(kind, head, me - way * step), RELAYED).start()

    for load, (kind, head) in zip(loads, chunks):
        load.wait()
        if kind == KEY and head == 0:
            load_q.start()

        @pl.when(me > 0)
        def _():
            send(-1, place(kind, head, me), OWN).start()

    if sides:
        @pl.when(source)
        def _():
            for i in range(len(ROUTES)):
                divert(i).start()

    @pl.when(me < n - 1)
    def _():
        pl.semaphore_wait(entered_sem, 1)
        for kind, head in chunks:
            send(1, place(kind, head, me), OWN).start()

    load_q.wait()
    load_order.wait()

    def low_first(block):
        return order_ref[2 * block] < order_ref[2 * block + 1]

    def low_span(block):
        return jnp.minimum(order_ref[2 * block], order_ref[2 * block + 1])

    def low_high(kind, block, head):
        at = place(kind, head, block)
        first, second = kv_ref[at, :span], kv_ref[at, span:]
        swap = low_first(block)
        return jnp.where(swap, first, second), jnp.where(swap, second, first)

    def score(queries, keys):
        return lax.dot_general(
            queries, keys, (((1,), (1,)), ((), ())), preferred_element_type=jnp.float32
        )

    def peak(scores):
        return jnp.broadcast_to(jnp.max(scores, axis=1, keepdims=True), (tall, HEAD_SIZE))

    def weights_of(scores, top):
        return jnp.exp2((scores - top) * exponent_scale).astype(jnp.bfloat16)

    mine_first = low_first(me)

    def stored(low, high):
        return jnp.where(mine_first, low, high), jnp.where(mine_first, high, low)

    def mixer(earlier, low, high):
        none = jnp.zeros_like(low)
        to_low = jnp.concatenate([none, jnp.where(earlier, low, none)], axis=0)
        to_high = jnp.concatenate([low, jnp.where(earlier, none, high)], axis=0)
        return jnp.concatenate(stored(to_low, to_high), axis=1)

    def product(weights, values):
        return jnp.dot(weights, values, preferred_element_type=jnp.float32)

    for head in range(kv_heads):
        for member in range(group):
            column = columns(head * group + member)
            low, high = stored(q_ref[:span, column], q_ref[span:, column])
            stack_ref[head, 0, member * span : (member + 1) * span] = low
            stack_ref[head, 1, member * span : (member + 1) * span] = high

    row = lax.rem(lax.broadcasted_iota(jnp.int32, (tall, span), 0), span)
    bias = jnp.where(lax.broadcasted_iota(jnp.int32, (tall, span), 1) <= row, 0.0, MASKED)
    ones = jnp.ones((span, HEAD_SIZE), jnp.bfloat16)
    for head in range(kv_heads):
        key_low, key_high = low_high(KEY, me, head)
        value_low, value_high = low_high(VALUE, me, head)
        low = score(stack_ref[head, 0], key_low) + bias
        low_top = peak(low)
        top_ref[head, 0] = low_top
        low = weights_of(low, low_top)
        cross = score(stack_ref[head, 1], key_low)
        high = score(stack_ref[head, 1], key_high) + bias
        high_top = jnp.maximum(peak(cross), peak(high))
        top_ref[head, 1] = high_top
        high = jnp.concatenate([weights_of(cross, high_top), weights_of(high, high_top)], axis=1)
        low = product(low, jnp.concatenate([value_low, ones], axis=1))
        high = product(high, jnp.concatenate(
            [jnp.concatenate([value_low, value_high], axis=0), jnp.concatenate([ones, ones], axis=0)], axis=1
        ))
        acc_ref[head] = jnp.concatenate(stored(low[:, :HEAD_SIZE], high[:, :HEAD_SIZE]), axis=1)
        sum_ref[head] = jnp.concatenate(stored(low[:, HEAD_SIZE:], high[:, HEAD_SIZE:]), axis=1)

    if sides:
        for i in range(len(ROUTES)):
            @pl.when(beside[i])
            def _():
                divert(i).wait_recv()
                rejoin(i).start()

    def weigh(block, head):
        earlier = low_span(block) < low_span(me)
        key_low, key_high = low_high(KEY, block, head)
        cross = score(stack_ref[head, 1], key_low)
        other = score(
            jnp.where(earlier, stack_ref[head, 0], stack_ref[head, 1]),
            jnp.where(earlier, key_low, key_high),
        )
        other_top = peak(other)
        old_low, old_high = top_ref[head, 0], top_ref[head, 1]
        low_top = jnp.maximum(old_low, jnp.where(earlier, other_top, MASKED))
        high_top = jnp.maximum(
            jnp.maximum(old_high, peak(cross)), jnp.where(earlier, MASKED, other_top)
        )
        top_ref[head, 0] = low_top
        top_ref[head, 1] = high_top
        weights = jnp.concatenate(
            [weights_of(cross, high_top), weights_of(other, jnp.where(earlier, low_top, high_top))], axis=1
        )
        p_ref[head] = weights
        fade = jnp.concatenate(
            stored(
                jnp.exp2((old_low - low_top) * exponent_scale),
                jnp.exp2((old_high - high_top) * exponent_scale),
            ),
            axis=1,
        )
        acc_ref[head] *= fade
        sum_ref[head] = sum_ref[head] * fade + product(weights, mixer(earlier, ones, ones))

    def gathered(block, head):
        earlier = low_span(block) < low_span(me)
        return acc_ref[head] + product(p_ref[head], mixer(earlier, *low_high(VALUE, block, head)))

    def turn(step, head):
        for way in (major, -major):
            @pl.when(inside(me - way * step))
            def _():
                arrive(way, KEY, head, step, way is major)
                weigh(me - way * step, head)
                arrive(way, VALUE, head, step, way is major)
                acc_ref[head] = gathered(me - way * step, head)

    def steps(step, carry):
        for head in range(kv_heads):
            turn(step, head)
        return carry

    lax.fori_loop(1, n - 1, steps, 0)


    def finish(head, total):
        result = (total * sum_ref[head]).astype(out_ref.dtype)
        for member in range(group):
            column = columns(head * group + member)
            part = slice(member * span, (member + 1) * span)
            out_ref[:span, column] = result[part, :HEAD_SIZE]
            out_ref[span:, column] = result[part, HEAD_SIZE:]

    last = me - major * (n - 1)
    for head in range(kv_heads):
        @pl.when(inside(last))
        def _():
            take(major, KEY, head, n - 1)
            weigh(last, head)
            sum_ref[head] = 1.0 / sum_ref[head]
            take(major, VALUE, head, n - 1)
            finish(head, gathered(last, head))

        @pl.when(jnp.logical_not(inside(last)))
        def _():
            sum_ref[head] = 1.0 / sum_ref[head]
            finish(head, acc_ref[head])

    if sides:
        @pl.when(source)
        def _():
            send(1, 0, DETOURED, 1).wait_send()
            divert(2).wait_send()

        @pl.when(beside[0] | beside[1] | beside[2])
        def _():
            rejoin(0).wait_send()

        @pl.when(spared)
        def _():
            send(1, 0, RELAYED, (n - 1) * per_block - 2).wait_send()
            remainder().wait_send()

    middle = (me > 0) & (me < n - 1)

    @pl.when(middle & jnp.logical_not(spared) if sides else middle)
    def _():
        send(1, 0, RELAYED, (n - 1) * per_block).wait_send()

    @pl.when(middle)
    def _():
        send(1, 0, OWN, 2 * per_block).wait_send()

    @pl.when(jnp.logical_not(middle))
    def _():
        send(1, 0, OWN, per_block).wait_send()


def shards(n, sides, queries, keys, values, span_order):
    rows, q_cols = queries.shape
    span = rows // 2
    kv_heads = keys.shape[1] // HEAD_SIZE
    tall = q_cols // HEAD_SIZE // kv_heads * span
    inputs = [pltpu.with_memory_space_constraint(x, pltpu.HBM) for x in (span_order, queries, keys, values)]
    return pl.pallas_call(
        functools.partial(attend, n, sides),
        out_shape=jax.ShapeDtypeStruct((rows, q_cols), jnp.bfloat16),
        in_specs=[pl.BlockSpec(memory_space=pltpu.HBM)] * 4,
        out_specs=pl.BlockSpec(memory_space=pltpu.VMEM),
        scratch_shapes=[
            pltpu.SMEM(span_order.shape, jnp.int32),
            pltpu.VMEM((rows, q_cols), jnp.bfloat16),
            pltpu.VMEM((2 * kv_heads * n, rows, HEAD_SIZE), jnp.bfloat16),
            pltpu.VMEM((rows // 2, HEAD_SIZE), jnp.bfloat16),
            pltpu.VMEM((kv_heads, 2, tall, HEAD_SIZE), jnp.bfloat16),
            pltpu.VMEM((kv_heads, tall, 2 * span), jnp.bfloat16),
            pltpu.VMEM((kv_heads, 2, tall, HEAD_SIZE), jnp.float32),
            pltpu.VMEM((kv_heads, tall, 2 * HEAD_SIZE), jnp.float32),
            pltpu.VMEM((kv_heads, tall, 2 * HEAD_SIZE), jnp.float32),
            pltpu.SemaphoreType.DMA((2 * kv_heads * n,)),
            pltpu.SemaphoreType.DMA((2,)),
            pltpu.SemaphoreType.DMA((4,)),
            pltpu.SemaphoreType.DMA,
            pltpu.SemaphoreType.REGULAR,
        ],
        compiler_params=pltpu.CompilerParams(
            collective_id=0, has_side_effects=True, vmem_limit_bytes=32 * 2**20
        ),
    )(*inputs)


def solution(mesh):
    split = P(("groups", "ctx"), ("head", "rep"))
    n = mesh.shape["ctx"]
    sides = n > 2 and min(mesh.shape[axis] for axis in SIDES + ("rep",)) > 1
    return jax.shard_map(
        functools.partial(shards, n, sides),
        mesh=mesh,
        in_specs=(split, split, split, P()),
        out_specs=split,
        check_vma=False,
    )
```

```python
import functools
import math

import jax
import jax.numpy as jnp
from jax import lax
from jax.experimental import pallas as pl
from jax.experimental.pallas import tpu as pltpu
from jax.sharding import PartitionSpec as P

HEAD_SIZE = 128
MASKED = -1e30
MESH = pl.DeviceIdType.MESH
KEY, VALUE = 0, 1
OWN, RELAYED = 0, 1
SIDES = ("groups", "head")
ROUTES = ((1, 0), (0, 1), (1, 1), (0, 0))


def columns(head):
    return pl.ds(head * HEAD_SIZE, HEAD_SIZE)


def product(weights, values):
    return jnp.dot(weights, values, preferred_element_type=jnp.float32)


def attend(n, sides, *refs):
    order_hbm, q_hbm, k_hbm, v_hbm = refs[:4]
    (
        acc_out, sum_out, p_out, mix_out,
        order_ref, q_ref, kv_ref, detour_ref, stack_ref, top_ref,
        chunk_sem, load_sem, send_sem, detour_sem, entered_sem,
    ) = refs[-15:]
    done_out, p_ref, sum_ref, acc_ref = refs[4:-15] or (None,) * 4
    me = lax.axis_index("ctx")
    rows, q_cols = q_ref.shape
    span = rows // 2
    kv_heads = k_hbm.shape[1] // HEAD_SIZE
    per_block = 2 * kv_heads
    group = q_cols // HEAD_SIZE // kv_heads
    tall = group * span
    half = rows // 2
    exponent_scale = math.log2(math.e) / math.sqrt(HEAD_SIZE)
    chunks = [(kind, head) for head in range(kv_heads) for kind in (KEY, VALUE)]
    tops = range(kv_heads)
    accs = [acc_ref.at[h] for h in tops[:-1]] + [acc_out]
    sums = [sum_ref.at[h] for h in tops[:-1]] + [sum_out]
    weights_refs = [p_ref.at[h] for h in tops[:-1]] + [p_out]

    def part(kind, head, block, start=0, count=rows):
        at = (block * per_block + 2 * head + kind) * rows + start
        return pl.ds(pl.multiple_of(at, half), count)

    def landing(kind, head, block, device):
        slot = lax.rem(block - device - 1 + n, n)
        return chunk_sem.at[slot * per_block + 2 * head + kind]

    def load(kind, head, sem):
        return pltpu.make_async_copy(
            (k_hbm, v_hbm)[kind].at[:, columns(head)], kv_ref.at[part(kind, head, me)], load_sem.at[sem]
        )

    load_order = pltpu.make_async_copy(order_hbm, order_ref, load_sem.at[1])
    load_q = pltpu.make_async_copy(q_hbm, q_ref, load_sem.at[0])
    load(*chunks[0], 0).start()
    for chunk in chunks[1:]:
        load(*chunk, 1).start()

    major = jnp.where(me < n // 2, -1, 1)

    def inside(index):
        return (index >= 0) & (index < n)

    barrier = pltpu.get_barrier_semaphore()

    @pl.when(me < n - 1)
    def _():
        pl.semaphore_signal(barrier, inc=1, device_id={"ctx": me + 1}, device_id_type=MESH)

    core = lax.axis_index("rep")

    def on_line(route):
        return (lax.axis_index(SIDES[0]) == route[0]) & (lax.axis_index(SIDES[1]) == route[1])

    def via(route):
        return {SIDES[0]: route[0], SIDES[1]: route[1], "rep": 1}

    ways_round = list(zip(ROUTES, [
        (KEY, kv_heads - 1, 0), (KEY, kv_heads - 1, half), (VALUE, kv_heads - 1, 0), (VALUE, 0, 0)
    ]))[: 3 if kv_heads == 1 else 4]
    corner = on_line((0, 0)) & (core == 0)
    source = corner & (me == n - 1)
    spared = corner & (me == 1)
    beside = [on_line(route) & (core == 1) & (me == n - 1) for route, _ in ways_round]
    helper = functools.reduce(jnp.logical_or, beside)
    if sides:
        @pl.when(corner & (me == 0))
        def _():
            for route, _ in ways_round:
                pl.semaphore_signal(
                    barrier, inc=1, device_id={"ctx": n - 1, **via(route)}, device_id_type=MESH
                )

        @pl.when(helper)
        def _():
            pl.semaphore_signal(
                barrier, inc=1, device_id={"groups": 0, "head": 0, "rep": 0}, device_id_type=MESH
            )

    @pl.when(me > 0)
    def _():
        others = jnp.where(source, len(ways_round), jnp.where(helper, 1, 0))
        pl.semaphore_wait(barrier, 1 + others if sides else 1)
        pl.semaphore_signal(entered_sem, inc=1, device_id={"ctx": me - 1}, device_id_type=MESH)

    def send(way, kind, head, block, pool, start=0, count=rows):
        target = jnp.clip(me + way, 0, n - 1)
        return pltpu.make_async_remote_copy(
            src_ref=kv_ref.at[part(kind, head, block, start, count)],
            dst_ref=kv_ref.at[part(kind, head, block, start, count)],
            send_sem=send_sem.at[pool],
            recv_sem=landing(kind, head, block, target),
            device_id={"ctx": target},
            device_id_type=MESH,
        )

    def sent(pool, count):
        everything = kv_ref.at[pl.ds(0, count)]
        pltpu.make_async_remote_copy(
            src_ref=everything,
            dst_ref=everything,
            send_sem=send_sem.at[pool],
            recv_sem=detour_sem,
            device_id={"ctx": me},
            device_id_type=MESH,
        ).wait_send()

    def take(way, kind, head, step):
        block = me - way * step
        pltpu.make_async_remote_copy(
            src_ref=kv_ref.at[part(kind, head, block)],
            dst_ref=kv_ref.at[part(kind, head, block)],
            send_sem=send_sem.at[RELAYED],
            recv_sem=landing(kind, head, block, me),
            device_id={"ctx": me},
            device_id_type=MESH,
        ).wait_recv()

    def divert(route, piece):
        kind, head, start = piece
        return pltpu.make_async_remote_copy(
            src_ref=kv_ref.at[part(kind, head, n - 1, start, half)],
            dst_ref=detour_ref,
            send_sem=send_sem.at[OWN],
            recv_sem=detour_sem,
            device_id=via(route),
            device_id_type=MESH,
        )

    def rejoin(piece):
        kind, head, start = piece
        return pltpu.make_async_remote_copy(
            src_ref=detour_ref,
            dst_ref=kv_ref.at[part(kind, head, n - 1, start, half)],
            send_sem=send_sem.at[OWN],
            recv_sem=landing(kind, head, n - 1, 0),
            device_id={"ctx": 0, "groups": 0, "head": 0, "rep": 0},
            device_id_type=MESH,
        )

    def arrive(way, kind, head, step, leading):
        take(way, kind, head, step)
        onward = inside(me + way)
        gone = [start for _, (*chunk, start) in ways_round if chunk == [kind, head]]
        if sides and leading and gone:
            last = spared & (step == n - 2)
            onward &= jnp.logical_not(last)
            if len(gone) == 1:
                @pl.when(last)
                def _():
                    send(-1, kind, head, me + step, RELAYED, half, half).start()

        @pl.when(onward)
        def _():
            send(way, kind, head, me - way * step, RELAYED).start()

    def send_own(way, kind, head):
        send(way, kind, head, me, OWN).start()

    load(*chunks[0], 0).wait()
    load_q.start()

    @pl.when(me > 0)
    def _():
        send_own(-1, *chunks[0])

    rest = kv_ref.at[part(VALUE, 0, me, 0, (per_block - 1) * rows)]
    pltpu.make_async_copy(rest, rest, load_sem.at[1]).wait()
    load_order.start()

    @pl.when(me > 0)
    def _():
        for chunk in chunks[1:]:
            send_own(-1, *chunk)

    if sides:
        @pl.when(source)
        def _():
            for route, piece in ways_round:
                divert(route, piece).start()

    @pl.when(me < n - 1)
    def _():
        pl.semaphore_wait(entered_sem, 1)
        for chunk in chunks:
            send_own(1, *chunk)

    load_q.wait()
    load_order.wait()

    def low_first(block):
        return order_ref[2 * block] < order_ref[2 * block + 1]

    def low_span(block):
        return jnp.minimum(order_ref[2 * block], order_ref[2 * block + 1])

    def low_high(kind, block, head):
        first = kv_ref[part(kind, head, block, 0, span)]
        second = kv_ref[part(kind, head, block, span, span)]
        swap = low_first(block)
        return jnp.where(swap, first, second), jnp.where(swap, second, first)

    def score(queries, keys):
        return lax.dot_general(
            queries, keys, (((1,), (1,)), ((), ())), preferred_element_type=jnp.float32
        )

    def peak(scores):
        return jnp.broadcast_to(jnp.max(scores, axis=1, keepdims=True), (tall, HEAD_SIZE))

    def weights_of(scores, top):
        return jnp.exp2((scores - top) * exponent_scale).astype(jnp.bfloat16)

    mine_first = low_first(me)

    def stored(low, high):
        return jnp.where(mine_first, low, high), jnp.where(mine_first, high, low)

    def mixer(earlier, low, high):
        none = jnp.zeros_like(low)
        to_low = jnp.concatenate([none, jnp.where(earlier, low, none)], axis=0)
        to_high = jnp.concatenate([low, jnp.where(earlier, none, high)], axis=0)
        return jnp.concatenate(stored(to_low, to_high), axis=1)

    for head in range(kv_heads):
        for member in range(group):
            column = columns(head * group + member)
            low, high = stored(q_ref[:span, column], q_ref[span:, column])
            stack_ref[head, 0, member * span : (member + 1) * span] = low
            stack_ref[head, 1, member * span : (member + 1) * span] = high

    row = lax.rem(lax.broadcasted_iota(jnp.int32, (tall, span), 0), span)
    bias = jnp.where(lax.broadcasted_iota(jnp.int32, (tall, span), 1) <= row, 0.0, MASKED)
    ones = jnp.ones((span, HEAD_SIZE), jnp.bfloat16)
    for head in range(kv_heads):
        key_low, key_high = low_high(KEY, me, head)
        value_low, value_high = low_high(VALUE, me, head)
        low = score(stack_ref[head, 0], key_low) + bias
        low_top = peak(low)
        top_ref[head, 0] = low_top
        low = weights_of(low, low_top)
        cross = score(stack_ref[head, 1], key_low)
        high = score(stack_ref[head, 1], key_high) + bias
        high_top = jnp.maximum(peak(cross), peak(high))
        top_ref[head, 1] = high_top
        high = jnp.concatenate([weights_of(cross, high_top), weights_of(high, high_top)], axis=1)
        low = product(low, jnp.concatenate([value_low, ones], axis=1))
        high = product(high, jnp.concatenate(
            [jnp.concatenate([value_low, value_high], axis=0), jnp.concatenate([ones, ones], axis=0)], axis=1
        ))
        accs[head][...] = jnp.concatenate(stored(low[:, :HEAD_SIZE], high[:, :HEAD_SIZE]), axis=1)
        sums[head][...] = jnp.concatenate(stored(low[:, HEAD_SIZE:], high[:, HEAD_SIZE:]), axis=1)

    if sides:
        for (route, piece), here in zip(ways_round, beside):
            @pl.when(here)
            def _():
                divert(route, piece).wait_recv()
                rejoin(piece).start()

    def weigh(block, head):
        earlier = low_span(block) < low_span(me)
        key_low, key_high = low_high(KEY, block, head)
        cross = score(stack_ref[head, 1], key_low)
        other = score(
            jnp.where(earlier, stack_ref[head, 0], stack_ref[head, 1]),
            jnp.where(earlier, key_low, key_high),
        )
        other_top = peak(other)
        old_low, old_high = top_ref[head, 0], top_ref[head, 1]
        low_top = jnp.maximum(old_low, jnp.where(earlier, other_top, MASKED))
        high_top = jnp.maximum(
            jnp.maximum(old_high, peak(cross)), jnp.where(earlier, MASKED, other_top)
        )
        top_ref[head, 0] = low_top
        top_ref[head, 1] = high_top
        weights = jnp.concatenate(
            [weights_of(cross, high_top), weights_of(other, jnp.where(earlier, low_top, high_top))], axis=1
        )
        weights_refs[head][...] = weights
        fade = jnp.concatenate(
            stored(
                jnp.exp2((old_low - low_top) * exponent_scale),
                jnp.exp2((old_high - high_top) * exponent_scale),
            ),
            axis=1,
        )
        accs[head][...] *= fade
        sums[head][...] = sums[head][...] * fade + product(weights, mixer(earlier, ones, ones))

    def mixed(block, head):
        return mixer(low_span(block) < low_span(me), *low_high(VALUE, block, head))

    def gathered(block, head):
        return accs[head][...] + product(weights_refs[head][...], mixed(block, head))

    def turn(step, head):
        for way in (major, -major):
            @pl.when(inside(me - way * step))
            def _():
                arrive(way, KEY, head, step, way is major)
                weigh(me - way * step, head)
                arrive(way, VALUE, head, step, way is major)
                accs[head][...] = gathered(me - way * step, head)

    def steps(step, carry):
        for head in range(kv_heads):
            turn(step, head)
        return carry

    lax.fori_loop(1, n - 1, steps, 0)

    def finish(head, total):
        place(done_out, head * group, span, (total * sums[head][...]).astype(jnp.bfloat16))

    last = me - major * (n - 1)
    for head in range(kv_heads - 1):
        @pl.when(inside(last))
        def _():
            take(major, KEY, head, n - 1)
            weigh(last, head)
            sums[head][...] = 1.0 / sums[head][...]
            take(major, VALUE, head, n - 1)
            finish(head, gathered(last, head))

        @pl.when(jnp.logical_not(inside(last)))
        def _():
            sums[head][...] = 1.0 / sums[head][...]
            finish(head, accs[head][...])

    @pl.when(inside(last))
    def _():
        take(major, KEY, kv_heads - 1, n - 1)
        weigh(last, kv_heads - 1)

    sum_out[...] = 1.0 / sum_out[...]

    middle = (me > 0) & (me < n - 1)

    @pl.when(middle)
    def _():
        sent(OWN, 2 * per_block * rows)
        mix_out[...] = jnp.zeros_like(mix_out)

    @pl.when(middle & jnp.logical_not(spared) if sides else middle)
    def _():
        sent(RELAYED, (n - 1) * per_block * rows)

    if sides:
        @pl.when(spared)
        def _():
            sent(RELAYED, (n - 1) * per_block * rows - len(ways_round) * half)

        @pl.when(source)
        def _():
            sent(OWN, per_block * rows + len(ways_round) * half)

        @pl.when(helper)
        def _():
            sent(OWN, per_block * rows + half)

    plain = jnp.logical_not(middle)
    if sides:
        plain &= jnp.logical_not(source | helper)

    @pl.when(plain)
    def _():
        sent(OWN, per_block * rows)

    @pl.when(inside(last))
    def _():
        take(major, VALUE, kv_heads - 1, n - 1)
        mix_out[...] = mixed(last, kv_heads - 1)


def place(ref, first, span, result):
    for member in range(result.shape[0] // span):
        block = result[member * span : (member + 1) * span]
        ref[:span, columns(first + member)] = block[:, :HEAD_SIZE]
        ref[span:, columns(first + member)] = block[:, HEAD_SIZE:]


def conclude(acc_ref, sum_ref, p_ref, mix_ref, *refs):
    out_hbm, stage_ref, sem = refs[-3:]
    done_refs = refs[:-3]
    span = stage_ref.shape[0] // 2
    group = acc_ref.shape[0] // span
    before = out_hbm.shape[1] // HEAD_SIZE - group
    for done_ref in done_refs:
        pltpu.make_async_copy(done_ref, out_hbm.at[:, pl.ds(0, before * HEAD_SIZE)], sem).start()
    for member in range(group):
        part = slice(member * span, (member + 1) * span)
        result = (acc_ref[part] + product(p_ref[part], mix_ref[...])) * sum_ref[part]
        place(stage_ref, member, span, result.astype(stage_ref.dtype))
        pltpu.make_async_copy(
            stage_ref.at[:, columns(member)], out_hbm.at[:, columns(before + member)], sem
        ).start()
    pltpu.make_async_copy(out_hbm, out_hbm, sem).wait()


def shards(n, sides, queries, keys, values, span_order):
    rows, q_cols = queries.shape
    span = rows // 2
    kv_heads = keys.shape[1] // HEAD_SIZE
    group = q_cols // HEAD_SIZE // kv_heads
    tall = group * span
    wide = 2 * HEAD_SIZE
    vmem = pl.BlockSpec(memory_space=pltpu.VMEM)
    inputs = [pltpu.with_memory_space_constraint(x, pltpu.HBM) for x in (span_order, queries, keys, values)]
    early = kv_heads - 1
    done = [jax.ShapeDtypeStruct((rows, early * group * HEAD_SIZE), jnp.bfloat16)] if early else []
    pending = [
        jax.ShapeDtypeStruct((tall, wide), jnp.float32),
        jax.ShapeDtypeStruct((tall, wide), jnp.float32),
        jax.ShapeDtypeStruct((tall, 2 * span), jnp.bfloat16),
        jax.ShapeDtypeStruct((2 * span, wide), jnp.bfloat16),
    ]
    early_scratch = [
        pltpu.VMEM((early, tall, 2 * span), jnp.bfloat16),
        pltpu.VMEM((early, tall, wide), jnp.float32),
        pltpu.VMEM((early, tall, wide), jnp.float32),
    ] if early else []

    def kernel(*refs):
        outs = len(done) + len(pending)
        ins, out, scratch = refs[:4], refs[4 : 4 + outs], refs[4 + outs :]
        extra = out[: len(done)] + scratch[: len(early_scratch)]
        attend(n, sides, *ins, *extra, *out[len(done) :], *scratch[len(early_scratch) :])

    results = pl.pallas_call(
        kernel,
        out_shape=done + pending,
        in_specs=[pl.BlockSpec(memory_space=pltpu.HBM)] * 4,
        out_specs=[vmem] * (len(done) + len(pending)),
        scratch_shapes=early_scratch + [
            pltpu.SMEM(span_order.shape, jnp.int32),
            pltpu.VMEM((rows, q_cols), jnp.bfloat16),
            pltpu.VMEM((2 * kv_heads * n * rows, HEAD_SIZE), jnp.bfloat16),
            pltpu.VMEM((rows // 2, HEAD_SIZE), jnp.bfloat16),
            pltpu.VMEM((kv_heads, 2, tall, HEAD_SIZE), jnp.bfloat16),
            pltpu.VMEM((kv_heads, 2, tall, HEAD_SIZE), jnp.float32),
            pltpu.SemaphoreType.DMA((2 * kv_heads * (n - 1),)),
            pltpu.SemaphoreType.DMA((2,)),
            pltpu.SemaphoreType.DMA((2,)),
            pltpu.SemaphoreType.DMA,
            pltpu.SemaphoreType.REGULAR,
        ],
        compiler_params=pltpu.CompilerParams(
            collective_id=0, has_side_effects=True, vmem_limit_bytes=32 * 2**20
        ),
    )(*inputs)
    operands = results[len(done) :] + results[: len(done)]
    return pl.pallas_call(
        conclude,
        out_shape=jax.ShapeDtypeStruct((rows, q_cols), jnp.bfloat16),
        in_specs=[vmem] * len(operands),
        out_specs=pl.BlockSpec(memory_space=pltpu.HBM),
        scratch_shapes=[
            pltpu.VMEM((rows, group * HEAD_SIZE), jnp.bfloat16),
            pltpu.SemaphoreType.DMA,
        ],
        compiler_params=pltpu.CompilerParams(vmem_limit_bytes=16 * 2**20),
    )(*operands)


def solution(mesh):
    split = P(("groups", "ctx"), ("head", "rep"))
    n = mesh.shape["ctx"]
    sides = n > 2 and min(mesh.shape[axis] for axis in SIDES + ("rep",)) > 1
    return jax.shard_map(
        functools.partial(shards, n, sides),
        mesh=mesh,
        in_specs=(split, split, split, P()),
        out_specs=split,
        check_vma=False,
    )
```

```python
import functools
import math

import jax
import jax.numpy as jnp
from jax import lax
from jax.experimental import pallas as pl
from jax.experimental.pallas import tpu as pltpu
from jax.sharding import PartitionSpec as P

HEAD_SIZE = 128
MASKED = -1e30
MESH = pl.DeviceIdType.MESH
KEY, VALUE = 0, 1
DIRECT = 1
OWN, RELAYED = 0, 1
SIDES = ("groups", "head")
ROUTES = ((1, 0), (0, 1), (1, 1), (0, 0))


def columns(head):
    return pl.ds(head * HEAD_SIZE, HEAD_SIZE)


def product(weights, values):
    return jnp.dot(weights, values, preferred_element_type=jnp.float32)


def attend(n, sides, *refs):
    order_hbm, q_hbm, k_hbm, v_hbm = refs[:4]
    (
        acc_out, sum_out, p_out, mix_out,
        order_ref, q_ref, kv_ref, detour_ref, stack_ref, top_ref,
        chunk_sem, load_sem, send_sem, detour_sem, entered_sem,
    ) = refs[-15:]
    done_out, p_ref, sum_ref, acc_ref = refs[4:-15] or (None,) * 4
    me = lax.axis_index("ctx")
    rows, q_cols = q_ref.shape
    span = rows // 2
    kv_heads = k_hbm.shape[1] // HEAD_SIZE
    per_block = 2 * kv_heads
    group = q_cols // HEAD_SIZE // kv_heads
    tall = group * span
    half = rows // 2
    exponent_scale = math.log2(math.e) / math.sqrt(HEAD_SIZE)
    chunks = [(kind, head) for head in range(kv_heads) for kind in (KEY, VALUE)]
    tops = range(kv_heads)
    accs = [acc_ref.at[h] for h in tops[:-1]] + [acc_out]
    sums = [sum_ref.at[h] for h in tops[:-1]] + [sum_out]
    weights_refs = [p_ref.at[h] for h in tops[:-1]] + [p_out]

    def part(kind, head, block, start=0, count=rows):
        at = (block * per_block + 2 * head + kind) * rows + start
        return pl.ds(pl.multiple_of(at, half), count)

    def landing(kind, head, block, device):
        slot = lax.rem(block - device - 1 + n, n)
        return chunk_sem.at[slot * per_block + 2 * head + kind]

    def load(kind, head, sem):
        return pltpu.make_async_copy(
            (k_hbm, v_hbm)[kind].at[:, columns(head)], kv_ref.at[part(kind, head, me)], load_sem.at[sem]
        )

    load_order = pltpu.make_async_copy(order_hbm, order_ref, load_sem.at[1])
    load_q = pltpu.make_async_copy(q_hbm, q_ref, load_sem.at[0])
    load(*chunks[0], 0).start()
    for chunk in chunks[1:]:
        load(*chunk, 1).start()

    major = jnp.where(me < n // 2, -1, 1)

    def inside(index):
        return (index >= 0) & (index < n)

    barrier = pltpu.get_barrier_semaphore()

    @pl.when(me < n - 1)
    def _():
        pl.semaphore_signal(barrier, inc=1, device_id={"ctx": me + 1}, device_id_type=MESH)

    core = lax.axis_index("rep")

    def on_line(route):
        return (lax.axis_index(SIDES[0]) == route[0]) & (lax.axis_index(SIDES[1]) == route[1])

    def via(route):
        return {SIDES[0]: route[0], SIDES[1]: route[1], "rep": 1}

    ways_round = list(zip(ROUTES, [
        (KEY, kv_heads - 1, 0), (KEY, kv_heads - 1, half), (VALUE, kv_heads - 1, 0), (VALUE, 0, 0)
    ]))[: 3 if kv_heads == 1 else 4]
    corner = on_line((0, 0)) & (core == 0)
    source = corner & (me == n - 1)
    spared = corner & (me == 1)
    beside = [on_line(route) & (core == 1) & (me == n - 1) for route, _ in ways_round]
    helper = functools.reduce(jnp.logical_or, beside)
    if sides:
        @pl.when(corner & (me == 0))
        def _():
            for route, _ in ways_round:
                pl.semaphore_signal(
                    barrier, inc=1, device_id={"ctx": n - 1, **via(route)}, device_id_type=MESH
                )

        @pl.when(helper)
        def _():
            pl.semaphore_signal(
                barrier, inc=1, device_id={"groups": 0, "head": 0, "rep": 0}, device_id_type=MESH
            )

    @pl.when(me > 0)
    def _():
        others = jnp.where(source, len(ways_round), jnp.where(helper, 1, 0))
        pl.semaphore_wait(barrier, 1 + others if sides else 1)
        pl.semaphore_signal(entered_sem, inc=1, device_id={"ctx": me - 1}, device_id_type=MESH)

    def send(way, kind, head, block, pool, start=0, count=rows):
        target = jnp.clip(me + way, 0, n - 1)
        return pltpu.make_async_remote_copy(
            src_ref=kv_ref.at[part(kind, head, block, start, count)],
            dst_ref=kv_ref.at[part(kind, head, block, start, count)],
            send_sem=send_sem.at[pool],
            recv_sem=landing(kind, head, block, target),
            device_id={"ctx": target},
            device_id_type=MESH,
        )

    def sent(pool, count):
        everything = kv_ref.at[pl.ds(0, count)]
        pltpu.make_async_remote_copy(
            src_ref=everything,
            dst_ref=everything,
            send_sem=send_sem.at[pool],
            recv_sem=detour_sem,
            device_id={"ctx": me},
            device_id_type=MESH,
        ).wait_send()

    def take(way, kind, head, step):
        block = me - way * step
        pltpu.make_async_remote_copy(
            src_ref=kv_ref.at[part(kind, head, block)],
            dst_ref=kv_ref.at[part(kind, head, block)],
            send_sem=send_sem.at[RELAYED],
            recv_sem=landing(kind, head, block, me),
            device_id={"ctx": me},
            device_id_type=MESH,
        ).wait_recv()

    def divert(route, piece):
        kind, head, start = piece
        return pltpu.make_async_remote_copy(
            src_ref=kv_ref.at[part(kind, head, n - 1, start, half)],
            dst_ref=detour_ref,
            send_sem=send_sem.at[OWN],
            recv_sem=detour_sem,
            device_id=via(route),
            device_id_type=MESH,
        )

    def rejoin(piece):
        kind, head, start = piece
        return pltpu.make_async_remote_copy(
            src_ref=detour_ref,
            dst_ref=kv_ref.at[part(kind, head, n - 1, start, half)],
            send_sem=send_sem.at[OWN],
            recv_sem=landing(kind, head, n - 1, 0),
            device_id={"ctx": 0, "groups": 0, "head": 0, "rep": 0},
            device_id_type=MESH,
        )

    def arrive(way, kind, head, step, leading):
        take(way, kind, head, step)
        onward = inside(me + way)
        gone = [start for _, (*chunk, start) in ways_round if chunk == [kind, head]]
        if sides and leading and gone:
            last = spared & (step == n - 2)
            onward &= jnp.logical_not(last)
            if len(gone) == 1:
                @pl.when(last)
                def _():
                    send(-1, kind, head, me + step, RELAYED, half, half).start()

        @pl.when(onward)
        def _():
            send(way, kind, head, me - way * step, RELAYED).start()

    def send_first(kind, head):
        return pltpu.make_async_remote_copy(
            src_ref=(k_hbm, v_hbm)[kind].at[:, columns(head)],
            dst_ref=kv_ref.at[part(kind, head, me)],
            send_sem=send_sem.at[OWN],
            recv_sem=landing(kind, head, me, jnp.maximum(me - 1, 0)),
            device_id={"ctx": jnp.maximum(me - 1, 0)},
            device_id_type=MESH,
        )

    def send_own(way, kind, head):
        send(way, kind, head, me, OWN).start()

    @pl.when(me > 0)
    def _():
        for chunk in chunks[:DIRECT]:
            send_first(*chunk).start()

    load(*chunks[0], 0).wait()
    load_q.start()

    rest = kv_ref.at[part(VALUE, 0, me, 0, (per_block - 1) * rows)]
    pltpu.make_async_copy(rest, rest, load_sem.at[1]).wait()
    load_order.start()

    @pl.when(me > 0)
    def _():
        for chunk in chunks[DIRECT:]:
            send_own(-1, *chunk)

    if sides:
        @pl.when(source)
        def _():
            for route, piece in ways_round:
                divert(route, piece).start()

    @pl.when(me < n - 1)
    def _():
        pl.semaphore_wait(entered_sem, 1)
        for chunk in chunks:
            send_own(1, *chunk)

    load_q.wait()
    load_order.wait()

    def low_first(block):
        return order_ref[2 * block] < order_ref[2 * block + 1]

    def low_span(block):
        return jnp.minimum(order_ref[2 * block], order_ref[2 * block + 1])

    def low_high(kind, block, head):
        first = kv_ref[part(kind, head, block, 0, span)]
        second = kv_ref[part(kind, head, block, span, span)]
        swap = low_first(block)
        return jnp.where(swap, first, second), jnp.where(swap, second, first)

    def score(queries, keys):
        return lax.dot_general(
            queries, keys, (((1,), (1,)), ((), ())), preferred_element_type=jnp.float32
        )

    def peak(scores):
        return jnp.broadcast_to(jnp.max(scores, axis=1, keepdims=True), (tall, HEAD_SIZE))

    def weights_of(scores, top):
        return jnp.exp2((scores - top) * exponent_scale).astype(jnp.bfloat16)

    mine_first = low_first(me)

    def stored(low, high):
        return jnp.where(mine_first, low, high), jnp.where(mine_first, high, low)

    def mixer(earlier, low, high):
        none = jnp.zeros_like(low)
        to_low = jnp.concatenate([none, jnp.where(earlier, low, none)], axis=0)
        to_high = jnp.concatenate([low, jnp.where(earlier, none, high)], axis=0)
        return jnp.concatenate(stored(to_low, to_high), axis=1)

    for head in range(kv_heads):
        for member in range(group):
            column = columns(head * group + member)
            low, high = stored(q_ref[:span, column], q_ref[span:, column])
            stack_ref[head, 0, member * span : (member + 1) * span] = low
            stack_ref[head, 1, member * span : (member + 1) * span] = high

    row = lax.rem(lax.broadcasted_iota(jnp.int32, (tall, span), 0), span)
    bias = jnp.where(lax.broadcasted_iota(jnp.int32, (tall, span), 1) <= row, 0.0, MASKED)
    ones = jnp.ones((span, HEAD_SIZE), jnp.bfloat16)
    for head in range(kv_heads):
        key_low, key_high = low_high(KEY, me, head)
        value_low, value_high = low_high(VALUE, me, head)
        low = score(stack_ref[head, 0], key_low) + bias
        low_top = peak(low)
        top_ref[head, 0] = low_top
        low = weights_of(low, low_top)
        cross = score(stack_ref[head, 1], key_low)
        high = score(stack_ref[head, 1], key_high) + bias
        high_top = jnp.maximum(peak(cross), peak(high))
        top_ref[head, 1] = high_top
        high = jnp.concatenate([weights_of(cross, high_top), weights_of(high, high_top)], axis=1)
        low = product(low, jnp.concatenate([value_low, ones], axis=1))
        high = product(high, jnp.concatenate(
            [jnp.concatenate([value_low, value_high], axis=0), jnp.concatenate([ones, ones], axis=0)], axis=1
        ))
        accs[head][...] = jnp.concatenate(stored(low[:, :HEAD_SIZE], high[:, :HEAD_SIZE]), axis=1)
        sums[head][...] = jnp.concatenate(stored(low[:, HEAD_SIZE:], high[:, HEAD_SIZE:]), axis=1)

    if sides:
        for (route, piece), here in zip(ways_round, beside):
            @pl.when(here)
            def _():
                divert(route, piece).wait_recv()
                rejoin(piece).start()

    def weigh(block, head):
        earlier = low_span(block) < low_span(me)
        key_low, key_high = low_high(KEY, block, head)
        cross = score(stack_ref[head, 1], key_low)
        other = score(
            jnp.where(earlier, stack_ref[head, 0], stack_ref[head, 1]),
            jnp.where(earlier, key_low, key_high),
        )
        other_top = peak(other)
        old_low, old_high = top_ref[head, 0], top_ref[head, 1]
        low_top = jnp.maximum(old_low, jnp.where(earlier, other_top, MASKED))
        high_top = jnp.maximum(
            jnp.maximum(old_high, peak(cross)), jnp.where(earlier, MASKED, other_top)
        )
        top_ref[head, 0] = low_top
        top_ref[head, 1] = high_top
        weights = jnp.concatenate(
            [weights_of(cross, high_top), weights_of(other, jnp.where(earlier, low_top, high_top))], axis=1
        )
        weights_refs[head][...] = weights
        fade = jnp.concatenate(
            stored(
                jnp.exp2((old_low - low_top) * exponent_scale),
                jnp.exp2((old_high - high_top) * exponent_scale),
            ),
            axis=1,
        )
        accs[head][...] *= fade
        sums[head][...] = sums[head][...] * fade + product(weights, mixer(earlier, ones, ones))

    def mixed(block, head):
        return mixer(low_span(block) < low_span(me), *low_high(VALUE, block, head))

    def gathered(block, head):
        return accs[head][...] + product(weights_refs[head][...], mixed(block, head))

    def turn(step, head):
        for way in (major, -major):
            @pl.when(inside(me - way * step))
            def _():
                arrive(way, KEY, head, step, way is major)
                weigh(me - way * step, head)
                arrive(way, VALUE, head, step, way is major)
                accs[head][...] = gathered(me - way * step, head)

    def steps(step, carry):
        for head in range(kv_heads):
            turn(step, head)
        return carry

    lax.fori_loop(1, n - 1, steps, 0)

    def finish(head, total):
        place(done_out, head * group, span, (total * sums[head][...]).astype(jnp.bfloat16))

    last = me - major * (n - 1)
    for head in range(kv_heads - 1):
        @pl.when(inside(last))
        def _():
            take(major, KEY, head, n - 1)
            weigh(last, head)
            sums[head][...] = 1.0 / sums[head][...]
            take(major, VALUE, head, n - 1)
            finish(head, gathered(last, head))

        @pl.when(jnp.logical_not(inside(last)))
        def _():
            sums[head][...] = 1.0 / sums[head][...]
            finish(head, accs[head][...])

    @pl.when(inside(last))
    def _():
        take(major, KEY, kv_heads - 1, n - 1)
        weigh(last, kv_heads - 1)

    sum_out[...] = 1.0 / sum_out[...]

    middle = (me > 0) & (me < n - 1)

    @pl.when(middle)
    def _():
        sent(OWN, 2 * per_block * rows)
        mix_out[...] = jnp.zeros_like(mix_out)

    @pl.when(middle & jnp.logical_not(spared) if sides else middle)
    def _():
        sent(RELAYED, (n - 1) * per_block * rows)

    if sides:
        @pl.when(spared)
        def _():
            sent(RELAYED, (n - 1) * per_block * rows - len(ways_round) * half)

        @pl.when(source)
        def _():
            sent(OWN, per_block * rows + len(ways_round) * half)

        @pl.when(helper)
        def _():
            sent(OWN, per_block * rows + half)

    plain = jnp.logical_not(middle)
    if sides:
        plain &= jnp.logical_not(source | helper)

    @pl.when(plain)
    def _():
        sent(OWN, per_block * rows)

    @pl.when(inside(last))
    def _():
        take(major, VALUE, kv_heads - 1, n - 1)
        mix_out[...] = mixed(last, kv_heads - 1)


def place(ref, first, span, result):
    for member in range(result.shape[0] // span):
        block = result[member * span : (member + 1) * span]
        ref[:span, columns(first + member)] = block[:, :HEAD_SIZE]
        ref[span:, columns(first + member)] = block[:, HEAD_SIZE:]


def conclude(acc_ref, sum_ref, p_ref, mix_ref, *refs):
    out_hbm, stage_ref, sem = refs[-3:]
    done_refs = refs[:-3]
    span = stage_ref.shape[0] // 2
    group = acc_ref.shape[0] // span
    before = out_hbm.shape[1] // HEAD_SIZE - group
    for done_ref in done_refs:
        pltpu.make_async_copy(done_ref, out_hbm.at[:, pl.ds(0, before * HEAD_SIZE)], sem).start()
    for member in range(group):
        part = slice(member * span, (member + 1) * span)
        result = (acc_ref[part] + product(p_ref[part], mix_ref[...])) * sum_ref[part]
        place(stage_ref, member, span, result.astype(stage_ref.dtype))
        pltpu.make_async_copy(
            stage_ref.at[:, columns(member)], out_hbm.at[:, columns(before + member)], sem
        ).start()
    pltpu.make_async_copy(out_hbm, out_hbm, sem).wait()


def shards(n, sides, queries, keys, values, span_order):
    rows, q_cols = queries.shape
    span = rows // 2
    kv_heads = keys.shape[1] // HEAD_SIZE
    group = q_cols // HEAD_SIZE // kv_heads
    tall = group * span
    wide = 2 * HEAD_SIZE
    vmem = pl.BlockSpec(memory_space=pltpu.VMEM)
    inputs = [pltpu.with_memory_space_constraint(x, pltpu.HBM) for x in (span_order, queries, keys, values)]
    early = kv_heads - 1
    done = [jax.ShapeDtypeStruct((rows, early * group * HEAD_SIZE), jnp.bfloat16)] if early else []
    pending = [
        jax.ShapeDtypeStruct((tall, wide), jnp.float32),
        jax.ShapeDtypeStruct((tall, wide), jnp.float32),
        jax.ShapeDtypeStruct((tall, 2 * span), jnp.bfloat16),
        jax.ShapeDtypeStruct((2 * span, wide), jnp.bfloat16),
    ]
    early_scratch = [
        pltpu.VMEM((early, tall, 2 * span), jnp.bfloat16),
        pltpu.VMEM((early, tall, wide), jnp.float32),
        pltpu.VMEM((early, tall, wide), jnp.float32),
    ] if early else []

    def kernel(*refs):
        outs = len(done) + len(pending)
        ins, out, scratch = refs[:4], refs[4 : 4 + outs], refs[4 + outs :]
        extra = out[: len(done)] + scratch[: len(early_scratch)]
        attend(n, sides, *ins, *extra, *out[len(done) :], *scratch[len(early_scratch) :])

    results = pl.pallas_call(
        kernel,
        out_shape=done + pending,
        in_specs=[pl.BlockSpec(memory_space=pltpu.HBM)] * 4,
        out_specs=[vmem] * (len(done) + len(pending)),
        scratch_shapes=early_scratch + [
            pltpu.SMEM(span_order.shape, jnp.int32),
            pltpu.VMEM((rows, q_cols), jnp.bfloat16),
            pltpu.VMEM((2 * kv_heads * n * rows, HEAD_SIZE), jnp.bfloat16),
            pltpu.VMEM((rows // 2, HEAD_SIZE), jnp.bfloat16),
            pltpu.VMEM((kv_heads, 2, tall, HEAD_SIZE), jnp.bfloat16),
            pltpu.VMEM((kv_heads, 2, tall, HEAD_SIZE), jnp.float32),
            pltpu.SemaphoreType.DMA((2 * kv_heads * (n - 1),)),
            pltpu.SemaphoreType.DMA((2,)),
            pltpu.SemaphoreType.DMA((2,)),
            pltpu.SemaphoreType.DMA,
            pltpu.SemaphoreType.REGULAR,
        ],
        compiler_params=pltpu.CompilerParams(
            collective_id=0, has_side_effects=True, vmem_limit_bytes=32 * 2**20
        ),
    )(*inputs)
    operands = results[len(done) :] + results[: len(done)]
    return pl.pallas_call(
        conclude,
        out_shape=jax.ShapeDtypeStruct((rows, q_cols), jnp.bfloat16),
        in_specs=[vmem] * len(operands),
        out_specs=pl.BlockSpec(memory_space=pltpu.HBM),
        scratch_shapes=[
            pltpu.VMEM((rows, group * HEAD_SIZE), jnp.bfloat16),
            pltpu.SemaphoreType.DMA,
        ],
        compiler_params=pltpu.CompilerParams(vmem_limit_bytes=16 * 2**20),
    )(*operands)


def solution(mesh):
    split = P(("groups", "ctx"), ("head", "rep"))
    n = mesh.shape["ctx"]
    sides = n > 2 and min(mesh.shape[axis] for axis in SIDES + ("rep",)) > 1
    return jax.shard_map(
        functools.partial(shards, n, sides),
        mesh=mesh,
        in_specs=(split, split, split, P()),
        out_specs=split,
        check_vma=False,
    )
```

```python
import functools
import math

import jax
import jax.numpy as jnp
from jax import lax
from jax.experimental import pallas as pl
from jax.experimental.pallas import tpu as pltpu
from jax.sharding import PartitionSpec as P

HEAD_SIZE = 128
MASKED = -1e30
MESH = pl.DeviceIdType.MESH
KEY, VALUE = 0, 1
DIRECT = 1
SIDES = ("groups", "head")
ROUTES = ((1, 0), (0, 1), (1, 1), (0, 0))


def columns(head):
    return pl.ds(head * HEAD_SIZE, HEAD_SIZE)


def product(weights, values):
    return jnp.dot(weights, values, preferred_element_type=jnp.float32)


def attend(n, sides, *refs):
    order_hbm, q_hbm, k_hbm, v_hbm = refs[:4]
    (
        acc_out, sum_out, p_out, mix_out,
        order_ref, q_ref, kv_ref, detour_ref, stack_ref, top_ref,
        chunk_sem, load_sem, send_sem, detour_sem, entered_sem,
    ) = refs[-15:]
    done_out, p_ref, sum_ref, acc_ref = refs[4:-15] or (None,) * 4
    me = lax.axis_index("ctx")
    rows, q_cols = q_ref.shape
    span = rows // 2
    kv_heads = k_hbm.shape[1] // HEAD_SIZE
    per_block = 2 * kv_heads
    group = q_cols // HEAD_SIZE // kv_heads
    tall = group * span
    half = rows // 2
    exponent_scale = math.log2(math.e) / math.sqrt(HEAD_SIZE)
    chunks = [(kind, head) for head in range(kv_heads) for kind in (KEY, VALUE)]
    tops = range(kv_heads)
    accs = [acc_ref.at[h] for h in tops[:-1]] + [acc_out]
    sums = [sum_ref.at[h] for h in tops[:-1]] + [sum_out]
    weights_refs = [p_ref.at[h] for h in tops[:-1]] + [p_out]

    def part(kind, head, block, start=0, count=rows):
        at = (block * per_block + 2 * head + kind) * rows + start
        return pl.ds(pl.multiple_of(at, 16), count)

    def landing(kind, head, block, device):
        slot = lax.rem(block - device - 1 + n, n)
        return chunk_sem.at[slot * per_block + 2 * head + kind]

    def load(kind, head, sem):
        return pltpu.make_async_copy(
            (k_hbm, v_hbm)[kind].at[:, columns(head)], kv_ref.at[part(kind, head, me)], load_sem.at[sem]
        )

    load_order = pltpu.make_async_copy(order_hbm, order_ref, load_sem.at[1])
    load_q = pltpu.make_async_copy(q_hbm, q_ref, load_sem.at[0])
    load(*chunks[0], 0).start()
    for chunk in chunks[1:]:
        load(*chunk, 1).start()

    major = jnp.where(me < n // 2, -1, 1)

    def inside(index):
        return (index >= 0) & (index < n)

    barrier = pltpu.get_barrier_semaphore()

    @pl.when(me < n - 1)
    def _():
        pl.semaphore_signal(barrier, inc=1, device_id={"ctx": me + 1}, device_id_type=MESH)

    core = lax.axis_index("rep")

    def on_line(route):
        return (lax.axis_index(SIDES[0]) == route[0]) & (lax.axis_index(SIDES[1]) == route[1])

    def via(route):
        return {SIDES[0]: route[0], SIDES[1]: route[1], "rep": 1}

    end = kv_heads - 1
    wide = rows * 7 // 16
    ways_round = [
        (ROUTES[0], [(KEY, end, 0, wide)]),
        (ROUTES[1], [(KEY, end, wide, wide)]),
        (ROUTES[2], [(KEY, end, 2 * wide, rows - 2 * wide), (VALUE, end, 0, 3 * half // 4)]),
    ]
    if kv_heads > 1:
        ways_round.append((ROUTES[3], [(VALUE, 0, 0, half)]))
    loads_round = [sum(count for *_, count in parts) for _, parts in ways_round]
    corner = on_line((0, 0)) & (core == 0)
    source = corner & (me == n - 1)
    spared = corner & (me == 1)
    beside = [on_line(route) & (core == 1) & (me == n - 1) for route, _ in ways_round]
    helper = functools.reduce(jnp.logical_or, beside)
    if sides:
        @pl.when(corner & (me == 0))
        def _():
            for route, _ in ways_round:
                pl.semaphore_signal(
                    barrier, inc=1, device_id={"ctx": n - 1, **via(route)}, device_id_type=MESH
                )

        @pl.when(helper)
        def _():
            pl.semaphore_signal(
                barrier, inc=1, device_id={"groups": 0, "head": 0, "rep": 0}, device_id_type=MESH
            )

    @pl.when(me > 0)
    def _():
        others = jnp.where(source, len(ways_round), jnp.where(helper, 1, 0))
        pl.semaphore_wait(barrier, 1 + others if sides else 1)
        pl.semaphore_signal(entered_sem, inc=1, device_id={"ctx": me - 1}, device_id_type=MESH)

    def send(way, kind, head, block, start=0, count=rows):
        target = jnp.clip(me + way, 0, n - 1)
        return pltpu.make_async_remote_copy(
            src_ref=kv_ref.at[part(kind, head, block, start, count)],
            dst_ref=kv_ref.at[part(kind, head, block, start, count)],
            send_sem=send_sem,
            recv_sem=landing(kind, head, block, target),
            device_id={"ctx": target},
            device_id_type=MESH,
        )

    def sent(count):
        everything = kv_ref.at[pl.ds(0, count)]
        pltpu.make_async_remote_copy(
            src_ref=everything,
            dst_ref=everything,
            send_sem=send_sem,
            recv_sem=detour_sem,
            device_id={"ctx": me},
            device_id_type=MESH,
        ).wait_send()

    def take(way, kind, head, step):
        block = me - way * step
        pltpu.make_async_remote_copy(
            src_ref=kv_ref.at[part(kind, head, block)],
            dst_ref=kv_ref.at[part(kind, head, block)],
            send_sem=send_sem,
            recv_sem=landing(kind, head, block, me),
            device_id={"ctx": me},
            device_id_type=MESH,
        ).wait_recv()

    def divert(route, parts):
        staged = 0
        for kind, head, start, count in parts:
            pltpu.make_async_remote_copy(
                src_ref=kv_ref.at[part(kind, head, n - 1, start, count)],
                dst_ref=detour_ref.at[pl.ds(staged, count)],
                send_sem=send_sem,
                recv_sem=detour_sem,
                device_id=via(route),
                device_id_type=MESH,
            ).start()
            staged += count

    def rejoin(parts):
        staged = sum(count for *_, count in parts)
        whole = detour_ref.at[pl.ds(0, staged)]
        pltpu.make_async_copy(whole, whole, detour_sem).wait()
        staged = 0
        for kind, head, start, count in parts:
            pltpu.make_async_remote_copy(
                src_ref=detour_ref.at[pl.ds(staged, count)],
                dst_ref=kv_ref.at[part(kind, head, n - 1, start, count)],
                send_sem=send_sem,
                recv_sem=landing(kind, head, n - 1, 0),
                device_id={"ctx": 0, "groups": 0, "head": 0, "rep": 0},
                device_id_type=MESH,
            ).start()
            staged += count

    def arrive(way, kind, head, step, leading):
        take(way, kind, head, step)
        onward = inside(me + way)
        gone = sum(
            count for _, parts in ways_round for *chunk, _, count in parts if chunk == [kind, head]
        )
        if sides and leading and gone:
            last = spared & (step == n - 2)
            onward &= jnp.logical_not(last)
            if gone < rows:
                @pl.when(last)
                def _():
                    send(-1, kind, head, me + step, gone, rows - gone).start()

        @pl.when(onward)
        def _():
            send(way, kind, head, me - way * step).start()

    def send_first(kind, head):
        return pltpu.make_async_remote_copy(
            src_ref=(k_hbm, v_hbm)[kind].at[:, columns(head)],
            dst_ref=kv_ref.at[part(kind, head, me)],
            send_sem=send_sem,
            recv_sem=landing(kind, head, me, jnp.maximum(me - 1, 0)),
            device_id={"ctx": jnp.maximum(me - 1, 0)},
            device_id_type=MESH,
        )

    def send_own(way, kind, head):
        send(way, kind, head, me).start()

    @pl.when(me > 0)
    def _():
        for chunk in chunks[:DIRECT]:
            send_first(*chunk).start()

    load(*chunks[0], 0).wait()
    load_q.start()

    rest = kv_ref.at[part(VALUE, 0, me, 0, (per_block - 1) * rows)]
    pltpu.make_async_copy(rest, rest, load_sem.at[1]).wait()
    load_order.start()

    @pl.when(me > 0)
    def _():
        for chunk in chunks[DIRECT:]:
            send_own(-1, *chunk)

    if sides:
        @pl.when(source)
        def _():
            for route, parts in ways_round:
                divert(route, parts)

    @pl.when(me < n - 1)
    def _():
        pl.semaphore_wait(entered_sem, 1)
        for chunk in chunks:
            send_own(1, *chunk)

    load_q.wait()
    load_order.wait()

    def low_first(block):
        return order_ref[2 * block] < order_ref[2 * block + 1]

    def low_span(block):
        return jnp.minimum(order_ref[2 * block], order_ref[2 * block + 1])

    def low_high(kind, block, head):
        first = kv_ref[part(kind, head, block, 0, span)]
        second = kv_ref[part(kind, head, block, span, span)]
        swap = low_first(block)
        return jnp.where(swap, first, second), jnp.where(swap, second, first)

    def score(queries, keys):
        return lax.dot_general(
            queries, keys, (((1,), (1,)), ((), ())), preferred_element_type=jnp.float32
        )

    def peak(scores):
        return jnp.broadcast_to(jnp.max(scores, axis=1, keepdims=True), (tall, HEAD_SIZE))

    def weights_of(scores, top):
        return jnp.exp2((scores - top) * exponent_scale).astype(jnp.bfloat16)

    mine_first = low_first(me)

    def stored(low, high):
        return jnp.where(mine_first, low, high), jnp.where(mine_first, high, low)

    def mixer(earlier, low, high):
        none = jnp.zeros_like(low)
        to_low = jnp.concatenate([none, jnp.where(earlier, low, none)], axis=0)
        to_high = jnp.concatenate([low, jnp.where(earlier, none, high)], axis=0)
        return jnp.concatenate(stored(to_low, to_high), axis=1)

    for head in range(kv_heads):
        for member in range(group):
            column = columns(head * group + member)
            low, high = stored(q_ref[:span, column], q_ref[span:, column])
            stack_ref[head, 0, member * span : (member + 1) * span] = low
            stack_ref[head, 1, member * span : (member + 1) * span] = high

    row = lax.rem(lax.broadcasted_iota(jnp.int32, (tall, span), 0), span)
    bias = jnp.where(lax.broadcasted_iota(jnp.int32, (tall, span), 1) <= row, 0.0, MASKED)
    ones = jnp.ones((span, HEAD_SIZE), jnp.bfloat16)
    for head in range(kv_heads):
        key_low, key_high = low_high(KEY, me, head)
        value_low, value_high = low_high(VALUE, me, head)
        low = score(stack_ref[head, 0], key_low) + bias
        low_top = peak(low)
        top_ref[head, 0] = low_top
        low = weights_of(low, low_top)
        cross = score(stack_ref[head, 1], key_low)
        high = score(stack_ref[head, 1], key_high) + bias
        high_top = jnp.maximum(peak(cross), peak(high))
        top_ref[head, 1] = high_top
        high = jnp.concatenate([weights_of(cross, high_top), weights_of(high, high_top)], axis=1)
        low = product(low, jnp.concatenate([value_low, ones], axis=1))
        high = product(high, jnp.concatenate(
            [jnp.concatenate([value_low, value_high], axis=0), jnp.concatenate([ones, ones], axis=0)], axis=1
        ))
        accs[head][...] = jnp.concatenate(stored(low[:, :HEAD_SIZE], high[:, :HEAD_SIZE]), axis=1)
        sums[head][...] = jnp.concatenate(stored(low[:, HEAD_SIZE:], high[:, HEAD_SIZE:]), axis=1)

    if sides:
        for (_, parts), here in zip(ways_round, beside):
            @pl.when(here)
            def _():
                rejoin(parts)

    def weigh(block, head):
        earlier = low_span(block) < low_span(me)
        key_low, key_high = low_high(KEY, block, head)
        cross = score(stack_ref[head, 1], key_low)
        other = score(
            jnp.where(earlier, stack_ref[head, 0], stack_ref[head, 1]),
            jnp.where(earlier, key_low, key_high),
        )
        other_top = peak(other)
        old_low, old_high = top_ref[head, 0], top_ref[head, 1]
        low_top = jnp.maximum(old_low, jnp.where(earlier, other_top, MASKED))
        high_top = jnp.maximum(
            jnp.maximum(old_high, peak(cross)), jnp.where(earlier, MASKED, other_top)
        )
        top_ref[head, 0] = low_top
        top_ref[head, 1] = high_top
        weights = jnp.concatenate(
            [weights_of(cross, high_top), weights_of(other, jnp.where(earlier, low_top, high_top))], axis=1
        )
        weights_refs[head][...] = weights
        fade = jnp.concatenate(
            stored(
                jnp.exp2((old_low - low_top) * exponent_scale),
                jnp.exp2((old_high - high_top) * exponent_scale),
            ),
            axis=1,
        )
        accs[head][...] *= fade
        sums[head][...] = sums[head][...] * fade + product(weights, mixer(earlier, ones, ones))

    def mixed(block, head):
        return mixer(low_span(block) < low_span(me), *low_high(VALUE, block, head))

    def gathered(block, head):
        return accs[head][...] + product(weights_refs[head][...], mixed(block, head))

    def turn(step, head):
        for way in (major, -major):
            @pl.when(inside(me - way * step))
            def _():
                arrive(way, KEY, head, step, way is major)
                weigh(me - way * step, head)
                arrive(way, VALUE, head, step, way is major)
                accs[head][...] = gathered(me - way * step, head)

    def steps(step, carry):
        for head in range(kv_heads):
            turn(step, head)
        return carry

    lax.fori_loop(1, n - 1, steps, 0)

    def finish(head, total):
        place(done_out, head * group, span, (total * sums[head][...]).astype(jnp.bfloat16))

    last = me - major * (n - 1)
    for head in range(kv_heads - 1):
        @pl.when(inside(last))
        def _():
            take(major, KEY, head, n - 1)
            weigh(last, head)
            sums[head][...] = 1.0 / sums[head][...]
            take(major, VALUE, head, n - 1)
            finish(head, gathered(last, head))

        @pl.when(jnp.logical_not(inside(last)))
        def _():
            sums[head][...] = 1.0 / sums[head][...]
            finish(head, accs[head][...])

    @pl.when(inside(last))
    def _():
        take(major, KEY, kv_heads - 1, n - 1)
        weigh(last, kv_heads - 1)

    sum_out[...] = 1.0 / sum_out[...]

    middle = (me > 0) & (me < n - 1)

    @pl.when(middle)
    def _():
        mix_out[...] = jnp.zeros_like(mix_out)

    @pl.when(middle & jnp.logical_not(spared) if sides else middle)
    def _():
        sent((n + 1) * per_block * rows)

    plain = jnp.logical_not(middle)
    if sides:
        @pl.when(spared)
        def _():
            sent((n + 1) * per_block * rows - sum(loads_round))

        @pl.when(source)
        def _():
            sent(per_block * rows + sum(loads_round))

        for count, here in zip(loads_round, beside):
            @pl.when(here)
            def _():
                sent(per_block * rows + count)

        plain &= jnp.logical_not(source | helper)

    @pl.when(plain)
    def _():
        sent(per_block * rows)

    @pl.when(inside(last))
    def _():
        take(major, VALUE, kv_heads - 1, n - 1)
        mix_out[...] = mixed(last, kv_heads - 1)


def place(ref, first, span, result):
    for member in range(result.shape[0] // span):
        block = result[member * span : (member + 1) * span]
        ref[:span, columns(first + member)] = block[:, :HEAD_SIZE]
        ref[span:, columns(first + member)] = block[:, HEAD_SIZE:]


def conclude(acc_ref, sum_ref, p_ref, mix_ref, *refs):
    out_hbm, stage_ref, sem = refs[-3:]
    done_refs = refs[:-3]
    span = stage_ref.shape[0] // 2
    group = acc_ref.shape[0] // span
    before = out_hbm.shape[1] // HEAD_SIZE - group
    for done_ref in done_refs:
        pltpu.make_async_copy(done_ref, out_hbm.at[:, pl.ds(0, before * HEAD_SIZE)], sem).start()
    for member in range(group):
        part = slice(member * span, (member + 1) * span)
        result = (acc_ref[part] + product(p_ref[part], mix_ref[...])) * sum_ref[part]
        place(stage_ref, member, span, result.astype(stage_ref.dtype))
        pltpu.make_async_copy(
            stage_ref.at[:, columns(member)], out_hbm.at[:, columns(before + member)], sem
        ).start()
    pltpu.make_async_copy(out_hbm, out_hbm, sem).wait()


def shards(n, sides, queries, keys, values, span_order):
    rows, q_cols = queries.shape
    span = rows // 2
    kv_heads = keys.shape[1] // HEAD_SIZE
    group = q_cols // HEAD_SIZE // kv_heads
    tall = group * span
    wide = 2 * HEAD_SIZE
    vmem = pl.BlockSpec(memory_space=pltpu.VMEM)
    inputs = [pltpu.with_memory_space_constraint(x, pltpu.HBM) for x in (span_order, queries, keys, values)]
    early = kv_heads - 1
    done = [jax.ShapeDtypeStruct((rows, early * group * HEAD_SIZE), jnp.bfloat16)] if early else []
    pending = [
        jax.ShapeDtypeStruct((tall, wide), jnp.float32),
        jax.ShapeDtypeStruct((tall, wide), jnp.float32),
        jax.ShapeDtypeStruct((tall, 2 * span), jnp.bfloat16),
        jax.ShapeDtypeStruct((2 * span, wide), jnp.bfloat16),
    ]
    early_scratch = [
        pltpu.VMEM((early, tall, 2 * span), jnp.bfloat16),
        pltpu.VMEM((early, tall, wide), jnp.float32),
        pltpu.VMEM((early, tall, wide), jnp.float32),
    ] if early else []

    def kernel(*refs):
        outs = len(done) + len(pending)
        ins, out, scratch = refs[:4], refs[4 : 4 + outs], refs[4 + outs :]
        extra = out[: len(done)] + scratch[: len(early_scratch)]
        attend(n, sides, *ins, *extra, *out[len(done) :], *scratch[len(early_scratch) :])

    results = pl.pallas_call(
        kernel,
        out_shape=done + pending,
        in_specs=[pl.BlockSpec(memory_space=pltpu.HBM)] * 4,
        out_specs=[vmem] * (len(done) + len(pending)),
        scratch_shapes=early_scratch + [
            pltpu.SMEM(span_order.shape, jnp.int32),
            pltpu.VMEM((rows, q_cols), jnp.bfloat16),
            pltpu.VMEM((2 * kv_heads * (n + 1) * rows, HEAD_SIZE), jnp.bfloat16),
            pltpu.VMEM((rows // 2, HEAD_SIZE), jnp.bfloat16),
            pltpu.VMEM((kv_heads, 2, tall, HEAD_SIZE), jnp.bfloat16),
            pltpu.VMEM((kv_heads, 2, tall, HEAD_SIZE), jnp.float32),
            pltpu.SemaphoreType.DMA((2 * kv_heads * (n - 1),)),
            pltpu.SemaphoreType.DMA((2,)),
            pltpu.SemaphoreType.DMA,
            pltpu.SemaphoreType.DMA,
            pltpu.SemaphoreType.REGULAR,
        ],
        compiler_params=pltpu.CompilerParams(
            collective_id=0, has_side_effects=True, vmem_limit_bytes=32 * 2**20
        ),
    )(*inputs)
    operands = results[len(done) :] + results[: len(done)]
    return pl.pallas_call(
        conclude,
        out_shape=jax.ShapeDtypeStruct((rows, q_cols), jnp.bfloat16),
        in_specs=[vmem] * len(operands),
        out_specs=pl.BlockSpec(memory_space=pltpu.HBM),
        scratch_shapes=[
            pltpu.VMEM((rows, group * HEAD_SIZE), jnp.bfloat16),
            pltpu.SemaphoreType.DMA,
        ],
        compiler_params=pltpu.CompilerParams(vmem_limit_bytes=16 * 2**20),
    )(*operands)


def solution(mesh):
    split = P(("groups", "ctx"), ("head", "rep"))
    n = mesh.shape["ctx"]
    sides = n > 3 and min(mesh.shape[axis] for axis in SIDES + ("rep",)) > 1
    return jax.shard_map(
        functools.partial(shards, n, sides),
        mesh=mesh,
        in_specs=(split, split, split, P()),
        out_specs=split,
        check_vma=False,
    )
```

```python
import functools
import math

import jax
import jax.numpy as jnp
from jax import lax
from jax.experimental import pallas as pl
from jax.experimental.pallas import tpu as pltpu
from jax.sharding import PartitionSpec as P

HEAD_SIZE = 128
MASKED = -1e30
MESH = pl.DeviceIdType.MESH
KEY, VALUE = 0, 1
DIRECT = 1
SIDES = ("groups", "head")
ROUTES = ((1, 0), (0, 1), (1, 1), (0, 0))


def columns(head):
    return pl.ds(head * HEAD_SIZE, HEAD_SIZE)


def product(weights, values):
    return jnp.dot(weights, values, preferred_element_type=jnp.float32)


def attend(n, sides, *refs):
    order_hbm, q_hbm, k_hbm, v_hbm = refs[:4]
    (
        acc_out, sum_out, p_out, mix_out,
        order_ref, q_ref, kv_ref, detour_ref, stack_ref, top_ref,
        chunk_sem, load_sem, send_sem, detour_sem, entered_sem,
    ) = refs[-15:]
    done_out, p_ref, sum_ref, acc_ref = refs[4:-15] or (None,) * 4
    me = lax.axis_index("ctx")
    rows, q_cols = q_ref.shape
    span = rows // 2
    kv_heads = k_hbm.shape[1] // HEAD_SIZE
    per_block = 2 * kv_heads
    group = q_cols // HEAD_SIZE // kv_heads
    tall = group * span
    half = rows // 2
    exponent_scale = math.log2(math.e) / math.sqrt(HEAD_SIZE)
    chunks = [(kind, head) for head in range(kv_heads) for kind in (KEY, VALUE)]
    tops = range(kv_heads)
    accs = [acc_ref.at[h] for h in tops[:-1]] + [acc_out]
    sums = [sum_ref.at[h] for h in tops[:-1]] + [sum_out]
    weights_refs = [p_ref.at[h] for h in tops[:-1]] + [p_out]

    def part(kind, head, block, start=0, count=rows):
        at = (block * per_block + 2 * head + kind) * rows + start
        return pl.ds(pl.multiple_of(at, 16), count)

    def landing(kind, head, block, device):
        slot = lax.rem(block - device - 1 + n, n)
        return chunk_sem.at[slot * per_block + 2 * head + kind]

    def load(kind, head, sem):
        return pltpu.make_async_copy(
            (k_hbm, v_hbm)[kind].at[:, columns(head)], kv_ref.at[part(kind, head, me)], load_sem.at[sem]
        )

    load_order = pltpu.make_async_copy(order_hbm, order_ref, load_sem.at[1])
    load_q = pltpu.make_async_copy(q_hbm, q_ref, load_sem.at[0])
    load(*chunks[0], 0).start()
    for chunk in chunks[1:]:
        load(*chunk, 1).start()

    major = jnp.where(me < n // 2, -1, 1)

    def inside(index):
        return (index >= 0) & (index < n)

    barrier = pltpu.get_barrier_semaphore()

    @pl.when(me < n - 1)
    def _():
        pl.semaphore_signal(barrier, inc=1, device_id={"ctx": me + 1}, device_id_type=MESH)

    core = lax.axis_index("rep")

    def on_line(route):
        return (lax.axis_index(SIDES[0]) == route[0]) & (lax.axis_index(SIDES[1]) == route[1])

    def via(route):
        return {SIDES[0]: route[0], SIDES[1]: route[1], "rep": 1}

    end = kv_heads - 1
    wide = half
    ways_round = [
        (ROUTES[0], [(KEY, end, 0, wide)]),
        (ROUTES[1], [(KEY, end, wide, wide)]),
        (ROUTES[2], [(VALUE, end, 0, half)]),
    ]
    if kv_heads > 1:
        ways_round.append((ROUTES[3], [(VALUE, 0, 0, half)]))
    loads_round = [sum(count for *_, count in parts) for _, parts in ways_round]
    corner = on_line((0, 0)) & (core == 0)
    source = corner & (me == n - 1)
    spared = corner & (me == 1)
    beside = [on_line(route) & (core == 1) & (me == n - 1) for route, _ in ways_round]
    helper = functools.reduce(jnp.logical_or, beside)
    if sides:
        @pl.when(corner & (me == 0))
        def _():
            for route, _ in ways_round:
                pl.semaphore_signal(
                    barrier, inc=1, device_id={"ctx": n - 1, **via(route)}, device_id_type=MESH
                )

        @pl.when(helper)
        def _():
            pl.semaphore_signal(
                barrier, inc=1, device_id={"groups": 0, "head": 0, "rep": 0}, device_id_type=MESH
            )

    @pl.when(me > 0)
    def _():
        others = jnp.where(source, len(ways_round), jnp.where(helper, 1, 0))
        pl.semaphore_wait(barrier, 1 + others if sides else 1)
        pl.semaphore_signal(entered_sem, inc=1, device_id={"ctx": me - 1}, device_id_type=MESH)

    def send(way, kind, head, block, start=0, count=rows):
        target = jnp.clip(me + way, 0, n - 1)
        return pltpu.make_async_remote_copy(
            src_ref=kv_ref.at[part(kind, head, block, start, count)],
            dst_ref=kv_ref.at[part(kind, head, block, start, count)],
            send_sem=send_sem,
            recv_sem=landing(kind, head, block, target),
            device_id={"ctx": target},
            device_id_type=MESH,
        )

    def sent(count):
        everything = kv_ref.at[pl.ds(0, count)]
        pltpu.make_async_remote_copy(
            src_ref=everything,
            dst_ref=everything,
            send_sem=send_sem,
            recv_sem=detour_sem,
            device_id={"ctx": me},
            device_id_type=MESH,
        ).wait_send()

    def take(way, kind, head, step):
        block = me - way * step
        pltpu.make_async_remote_copy(
            src_ref=kv_ref.at[part(kind, head, block)],
            dst_ref=kv_ref.at[part(kind, head, block)],
            send_sem=send_sem,
            recv_sem=landing(kind, head, block, me),
            device_id={"ctx": me},
            device_id_type=MESH,
        ).wait_recv()

    def divert(route, parts):
        staged = 0
        for kind, head, start, count in parts:
            pltpu.make_async_remote_copy(
                src_ref=kv_ref.at[part(kind, head, n - 1, start, count)],
                dst_ref=detour_ref.at[pl.ds(staged, count)],
                send_sem=send_sem,
                recv_sem=detour_sem,
                device_id=via(route),
                device_id_type=MESH,
            ).start()
            staged += count

    def rejoin(parts):
        staged = sum(count for *_, count in parts)
        whole = detour_ref.at[pl.ds(0, staged)]
        pltpu.make_async_copy(whole, whole, detour_sem).wait()
        staged = 0
        for kind, head, start, count in parts:
            pltpu.make_async_remote_copy(
                src_ref=detour_ref.at[pl.ds(staged, count)],
                dst_ref=kv_ref.at[part(kind, head, n - 1, start, count)],
                send_sem=send_sem,
                recv_sem=landing(kind, head, n - 1, 0),
                device_id={"ctx": 0, "groups": 0, "head": 0, "rep": 0},
                device_id_type=MESH,
            ).start()
            staged += count

    def arrive(way, kind, head, step, leading):
        take(way, kind, head, step)
        onward = inside(me + way)
        gone = sum(
            count for _, parts in ways_round for *chunk, _, count in parts if chunk == [kind, head]
        )
        if sides and leading and gone:
            last = spared & (step == n - 2)
            onward &= jnp.logical_not(last)
            if gone < rows:
                @pl.when(last)
                def _():
                    send(-1, kind, head, me + step, gone, rows - gone).start()

        @pl.when(onward)
        def _():
            send(way, kind, head, me - way * step).start()

    def send_first(kind, head):
        return pltpu.make_async_remote_copy(
            src_ref=(k_hbm, v_hbm)[kind].at[:, columns(head)],
            dst_ref=kv_ref.at[part(kind, head, me)],
            send_sem=send_sem,
            recv_sem=landing(kind, head, me, jnp.maximum(me - 1, 0)),
            device_id={"ctx": jnp.maximum(me - 1, 0)},
            device_id_type=MESH,
        )

    def send_own(way, kind, head):
        send(way, kind, head, me).start()

    @pl.when(me > 0)
    def _():
        for chunk in chunks[:DIRECT]:
            send_first(*chunk).start()

    load(*chunks[0], 0).wait()
    load_q.start()

    rest = kv_ref.at[part(VALUE, 0, me, 0, (per_block - 1) * rows)]
    pltpu.make_async_copy(rest, rest, load_sem.at[1]).wait()
    load_order.start()

    @pl.when(me > 0)
    def _():
        for chunk in chunks[DIRECT:]:
            send_own(-1, *chunk)

    if sides:
        @pl.when(source)
        def _():
            for route, parts in ways_round:
                divert(route, parts)

    @pl.when(me < n - 1)
    def _():
        pl.semaphore_wait(entered_sem, 1)
        for chunk in chunks:
            send_own(1, *chunk)

    load_q.wait()
    load_order.wait()

    def low_first(block):
        return order_ref[2 * block] < order_ref[2 * block + 1]

    def low_span(block):
        return jnp.minimum(order_ref[2 * block], order_ref[2 * block + 1])

    def low_high(kind, block, head):
        first = kv_ref[part(kind, head, block, 0, span)]
        second = kv_ref[part(kind, head, block, span, span)]
        swap = low_first(block)
        return jnp.where(swap, first, second), jnp.where(swap, second, first)

    def score(queries, keys):
        return lax.dot_general(
            queries, keys, (((1,), (1,)), ((), ())), preferred_element_type=jnp.float32
        )

    def peak(scores):
        return jnp.broadcast_to(jnp.max(scores, axis=1, keepdims=True), (tall, HEAD_SIZE))

    def weights_of(scores, top):
        return jnp.exp2((scores - top) * exponent_scale).astype(jnp.bfloat16)

    mine_first = low_first(me)

    def stored(low, high):
        return jnp.where(mine_first, low, high), jnp.where(mine_first, high, low)

    def mixer(earlier, low, high):
        none = jnp.zeros_like(low)
        to_low = jnp.concatenate([none, jnp.where(earlier, low, none)], axis=0)
        to_high = jnp.concatenate([low, jnp.where(earlier, none, high)], axis=0)
        return jnp.concatenate(stored(to_low, to_high), axis=1)

    for head in range(kv_heads):
        for member in range(group):
            column = columns(head * group + member)
            low, high = stored(q_ref[:span, column], q_ref[span:, column])
            stack_ref[head, 0, member * span : (member + 1) * span] = low
            stack_ref[head, 1, member * span : (member + 1) * span] = high

    row = lax.rem(lax.broadcasted_iota(jnp.int32, (tall, span), 0), span)
    bias = jnp.where(lax.broadcasted_iota(jnp.int32, (tall, span), 1) <= row, 0.0, MASKED)
    ones = jnp.ones((span, HEAD_SIZE), jnp.bfloat16)
    for head in range(kv_heads):
        key_low, key_high = low_high(KEY, me, head)
        value_low, value_high = low_high(VALUE, me, head)
        low = score(stack_ref[head, 0], key_low) + bias
        low_top = peak(low)
        top_ref[head, 0] = low_top
        low = weights_of(low, low_top)
        cross = score(stack_ref[head, 1], key_low)
        high = score(stack_ref[head, 1], key_high) + bias
        high_top = jnp.maximum(peak(cross), peak(high))
        top_ref[head, 1] = high_top
        high = jnp.concatenate([weights_of(cross, high_top), weights_of(high, high_top)], axis=1)
        low = product(low, jnp.concatenate([value_low, ones], axis=1))
        high = product(high, jnp.concatenate(
            [jnp.concatenate([value_low, value_high], axis=0), jnp.concatenate([ones, ones], axis=0)], axis=1
        ))
        accs[head][...] = jnp.concatenate(stored(low[:, :HEAD_SIZE], high[:, :HEAD_SIZE]), axis=1)
        sums[head][...] = jnp.concatenate(stored(low[:, HEAD_SIZE:], high[:, HEAD_SIZE:]), axis=1)

    if sides:
        for (_, parts), here in zip(ways_round, beside):
            @pl.when(here)
            def _():
                rejoin(parts)

    def weigh(block, head):
        earlier = low_span(block) < low_span(me)
        key_low, key_high = low_high(KEY, block, head)
        cross = score(stack_ref[head, 1], key_low)
        other = score(
            jnp.where(earlier, stack_ref[head, 0], stack_ref[head, 1]),
            jnp.where(earlier, key_low, key_high),
        )
        other_top = peak(other)
        old_low, old_high = top_ref[head, 0], top_ref[head, 1]
        low_top = jnp.maximum(old_low, jnp.where(earlier, other_top, MASKED))
        high_top = jnp.maximum(
            jnp.maximum(old_high, peak(cross)), jnp.where(earlier, MASKED, other_top)
        )
        top_ref[head, 0] = low_top
        top_ref[head, 1] = high_top
        weights = jnp.concatenate(
            [weights_of(cross, high_top), weights_of(other, jnp.where(earlier, low_top, high_top))], axis=1
        )
        weights_refs[head][...] = weights
        fade = jnp.concatenate(
            stored(
                jnp.exp2((old_low - low_top) * exponent_scale),
                jnp.exp2((old_high - high_top) * exponent_scale),
            ),
            axis=1,
        )
        accs[head][...] *= fade
        sums[head][...] = sums[head][...] * fade + product(weights, mixer(earlier, ones, ones))

    def mixed(block, head):
        return mixer(low_span(block) < low_span(me), *low_high(VALUE, block, head))

    def gathered(block, head):
        return accs[head][...] + product(weights_refs[head][...], mixed(block, head))

    def turn(step, head):
        for way in (major, -major):
            @pl.when(inside(me - way * step))
            def _():
                arrive(way, KEY, head, step, way is major)
                weigh(me - way * step, head)
                arrive(way, VALUE, head, step, way is major)
                accs[head][...] = gathered(me - way * step, head)

    def steps(step, carry):
        for head in range(kv_heads):
            turn(step, head)
        return carry

    lax.fori_loop(1, n - 1, steps, 0)

    def finish(head, total):
        place(done_out, head * group, span, (total * sums[head][...]).astype(jnp.bfloat16))

    last = me - major * (n - 1)
    for head in range(kv_heads - 1):
        @pl.when(inside(last))
        def _():
            take(major, KEY, head, n - 1)
            weigh(last, head)
            sums[head][...] = 1.0 / sums[head][...]
            take(major, VALUE, head, n - 1)
            finish(head, gathered(last, head))

        @pl.when(jnp.logical_not(inside(last)))
        def _():
            sums[head][...] = 1.0 / sums[head][...]
            finish(head, accs[head][...])

    @pl.when(inside(last))
    def _():
        take(major, KEY, kv_heads - 1, n - 1)
        weigh(last, kv_heads - 1)

    sum_out[...] = 1.0 / sum_out[...]

    middle = (me > 0) & (me < n - 1)

    @pl.when(middle)
    def _():
        mix_out[...] = jnp.zeros_like(mix_out)

    @pl.when(middle & jnp.logical_not(spared) if sides else middle)
    def _():
        sent((n + 1) * per_block * rows)

    plain = jnp.logical_not(middle)
    if sides:
        @pl.when(spared)
        def _():
            sent((n + 1) * per_block * rows - sum(loads_round))

        @pl.when(source)
        def _():
            sent(per_block * rows + sum(loads_round))

        for count, here in zip(loads_round, beside):
            @pl.when(here)
            def _():
                sent(per_block * rows + count)

        plain &= jnp.logical_not(source | helper)

    @pl.when(plain)
    def _():
        sent(per_block * rows)

    @pl.when(inside(last))
    def _():
        take(major, VALUE, kv_heads - 1, n - 1)
        mix_out[...] = mixed(last, kv_heads - 1)


def place(ref, first, span, result):
    for member in range(result.shape[0] // span):
        block = result[member * span : (member + 1) * span]
        ref[:span, columns(first + member)] = block[:, :HEAD_SIZE]
        ref[span:, columns(first + member)] = block[:, HEAD_SIZE:]


def conclude(acc_ref, sum_ref, p_ref, mix_ref, *refs):
    out_hbm, stage_ref, sem = refs[-3:]
    done_refs = refs[:-3]
    span = stage_ref.shape[0] // 2
    group = acc_ref.shape[0] // span
    before = out_hbm.shape[1] // HEAD_SIZE - group
    for done_ref in done_refs:
        pltpu.make_async_copy(done_ref, out_hbm.at[:, pl.ds(0, before * HEAD_SIZE)], sem).start()
    for member in range(group):
        part = slice(member * span, (member + 1) * span)
        result = (acc_ref[part] + product(p_ref[part], mix_ref[...])) * sum_ref[part]
        place(stage_ref, member, span, result.astype(stage_ref.dtype))
        pltpu.make_async_copy(
            stage_ref.at[:, columns(member)], out_hbm.at[:, columns(before + member)], sem
        ).start()
    pltpu.make_async_copy(out_hbm, out_hbm, sem).wait()


def shards(n, sides, queries, keys, values, span_order):
    rows, q_cols = queries.shape
    span = rows // 2
    kv_heads = keys.shape[1] // HEAD_SIZE
    group = q_cols // HEAD_SIZE // kv_heads
    tall = group * span
    wide = 2 * HEAD_SIZE
    vmem = pl.BlockSpec(memory_space=pltpu.VMEM)
    inputs = [pltpu.with_memory_space_constraint(x, pltpu.HBM) for x in (span_order, queries, keys, values)]
    early = kv_heads - 1
    done = [jax.ShapeDtypeStruct((rows, early * group * HEAD_SIZE), jnp.bfloat16)] if early else []
    pending = [
        jax.ShapeDtypeStruct((tall, wide), jnp.float32),
        jax.ShapeDtypeStruct((tall, wide), jnp.float32),
        jax.ShapeDtypeStruct((tall, 2 * span), jnp.bfloat16),
        jax.ShapeDtypeStruct((2 * span, wide), jnp.bfloat16),
    ]
    early_scratch = [
        pltpu.VMEM((early, tall, 2 * span), jnp.bfloat16),
        pltpu.VMEM((early, tall, wide), jnp.float32),
        pltpu.VMEM((early, tall, wide), jnp.float32),
    ] if early else []

    def kernel(*refs):
        outs = len(done) + len(pending)
        ins, out, scratch = refs[:4], refs[4 : 4 + outs], refs[4 + outs :]
        extra = out[: len(done)] + scratch[: len(early_scratch)]
        attend(n, sides, *ins, *extra, *out[len(done) :], *scratch[len(early_scratch) :])

    results = pl.pallas_call(
        kernel,
        out_shape=done + pending,
        in_specs=[pl.BlockSpec(memory_space=pltpu.HBM)] * 4,
        out_specs=[vmem] * (len(done) + len(pending)),
        scratch_shapes=early_scratch + [
            pltpu.SMEM(span_order.shape, jnp.int32),
            pltpu.VMEM((rows, q_cols), jnp.bfloat16),
            pltpu.VMEM((2 * kv_heads * (n + 1) * rows, HEAD_SIZE), jnp.bfloat16),
            pltpu.VMEM((rows // 2, HEAD_SIZE), jnp.bfloat16),
            pltpu.VMEM((kv_heads, 2, tall, HEAD_SIZE), jnp.bfloat16),
            pltpu.VMEM((kv_heads, 2, tall, HEAD_SIZE), jnp.float32),
            pltpu.SemaphoreType.DMA((2 * kv_heads * (n - 1),)),
            pltpu.SemaphoreType.DMA((2,)),
            pltpu.SemaphoreType.DMA,
            pltpu.SemaphoreType.DMA,
            pltpu.SemaphoreType.REGULAR,
        ],
        compiler_params=pltpu.CompilerParams(
            collective_id=0, has_side_effects=True, vmem_limit_bytes=32 * 2**20
        ),
    )(*inputs)
    operands = results[len(done) :] + results[: len(done)]
    return pl.pallas_call(
        conclude,
        out_shape=jax.ShapeDtypeStruct((rows, q_cols), jnp.bfloat16),
        in_specs=[vmem] * len(operands),
        out_specs=pl.BlockSpec(memory_space=pltpu.HBM),
        scratch_shapes=[
            pltpu.VMEM((rows, group * HEAD_SIZE), jnp.bfloat16),
            pltpu.SemaphoreType.DMA,
        ],
        compiler_params=pltpu.CompilerParams(vmem_limit_bytes=16 * 2**20),
    )(*operands)


def solution(mesh):
    split = P(("groups", "ctx"), ("head", "rep"))
    n = mesh.shape["ctx"]
    sides = n > 3 and min(mesh.shape[axis] for axis in SIDES + ("rep",)) > 1
    return jax.shard_map(
        functools.partial(shards, n, sides),
        mesh=mesh,
        in_specs=(split, split, split, P()),
        out_specs=split,
        check_vma=False,
    )
```
